32 devices in a mesh: dp: 4 (over x, y), sp: 8 (over z, core).
Axes of the slice: x: 2, y: 2, z: 4, core: 2. Of those that a mesh axis runs over, the one named last changes fastest.
Arguments:
- x: bfloat16 [4096, 4096], P(('dp', 'sp')), parts along dimension 0
- gain: bfloat16 [4096], replicated
- wq: bfloat16 [4096, 4096], replicated
- wk: bfloat16 [4096, 256], replicated
- wv: bfloat16 [4096, 256], replicated
- wo: bfloat16 [4096, 4096], replicated
Outputs:
- output: bfloat16 [4096, 4096], P(('dp', 'sp')), parts along dimension 0
There are 4 independent parts. The reference program is written for one: setup_inputs(seed, part) draws one part's arguments, and reference() takes and returns one part's arrays. A program takes and returns all parts, laid end to end along the dimension named above; an argument that names none is the same for every part.
All inputs are finite; a program needn't handle non-finite values.
Results may differ from the reference program's by a relative error of at most 0.012.
Values are sent between devices in bfloat16 or wider.
A program may use at most 2 GiB of HBM per device.

```python
import jax
import jax.numpy as jnp
from jax import lax

ROWS = 1024
D = 4096
HEADS = 32
KV_HEADS = 2
HEAD = 128
THETA = 10000


def setup_inputs(seed: int = 0, part: int = 0) -> dict:
    kx, kn, kq, kk, kv, ko = jax.random.split(jax.random.key(seed), 6)

    def weights(key, rows, columns):
        return jax.random.normal(key, (rows, columns), jnp.float32) * rows**-0.5

    drawn = {
        "x": jax.random.normal(jax.random.fold_in(kx, part), (ROWS, D), jnp.float32),
        "gain": 1 + 0.1 * jax.random.normal(kn, (D,), jnp.float32),
        "wq": 2 * weights(kq, D, HEADS * HEAD),
        "wk": 2 * weights(kk, D, KV_HEADS * HEAD),
        "wv": 4 * weights(kv, D, KV_HEADS * HEAD),
        "wo": weights(ko, HEADS * HEAD, D),
    }
    return {k: v.astype(jnp.bfloat16) for k, v in drawn.items()}


def normed(x, gain):
    wide = x.astype(jnp.float32)
    scale = lax.rsqrt(jnp.mean(wide * wide, -1, keepdims=True) + 1e-6)
    return (wide * scale * gain.astype(jnp.float32)).astype(jnp.bfloat16)


def turned(t, place, theta):
    half = t.shape[-1] // 2
    angle = place.astype(jnp.float32)[:, None] * theta ** (-jnp.arange(half, dtype=jnp.float32) / half)
    cos, sin = jnp.cos(angle)[:, None], jnp.sin(angle)[:, None]
    a, b = t[..., :half].astype(jnp.float32), t[..., half:].astype(jnp.float32)
    return jnp.concatenate([a * cos - b * sin, b * cos + a * sin], -1).astype(jnp.bfloat16)


def matmul(a, w):
    return jnp.dot(a, w, preferred_element_type=jnp.float32).astype(jnp.bfloat16)


def einsum(form, a, b):
    return jnp.einsum(form, a.astype(jnp.float32), b.astype(jnp.float32))


def attention(q, k, v):
    scores = einsum("tgsd,ugd->gstu", q, k) * q.shape[-1] ** -0.5
    token = jnp.arange(q.shape[0])
    scores = jnp.where(token[:, None] >= token, scores, -jnp.inf)
    weights = jax.nn.softmax(scores, -1).astype(jnp.bfloat16)
    return einsum("gstu,ugd->tgsd", weights, v).astype(jnp.bfloat16)


def reference(x, gain, wq, wk, wv, wo):
    a, place = normed(x, gain), jnp.arange(ROWS)
    q = turned(matmul(a, wq).reshape(ROWS, HEADS, HEAD), place, THETA).reshape(ROWS, KV_HEADS, -1, HEAD)
    k = turned(matmul(a, wk).reshape(ROWS, KV_HEADS, HEAD), place, THETA)
    v = matmul(a, wv).reshape(ROWS, KV_HEADS, HEAD)
    seen = attention(q, k, v).reshape(ROWS, HEADS * HEAD)
    return (x.astype(jnp.float32) + jnp.dot(seen, wo, preferred_element_type=jnp.float32)).astype(jnp.bfloat16)
```

```python
import functools
import math

import jax
import jax.numpy as jnp
import numpy as np
from jax import lax
from jax.experimental import pallas as pl
from jax.experimental.pallas import tpu as pltpu
from jax.sharding import PartitionSpec as P

HEAD = 128
THETA = 10000
HIDDEN = -2e30
LOG2E = 1.4426950408889634
MESH = pl.DeviceIdType.MESH
F32, BF16 = jnp.float32, jnp.bfloat16
T = 128
C = 2 * T
W = 512
Z = 4
QH = 16


def _dot(a, b, ca=1, cb=0):
    return lax.dot_general(a, b, (((ca,), (cb,)), ((), ())), preferred_element_type=F32)


def _turn(t, cos, sin):
    return (t * cos + pltpu.roll(t, HEAD // 2, 1) * sin).astype(BF16)


def _kernel(x_ref, g_ref, wq_ref, wk_ref, wv_ref, wo_ref, tab_ref, y_ref,
            xb, a_s, wk_s, wv_s, wq_s, wo_s, cs, q_s, kvb, kvo, top_s, mix_s, at_own, at_par, acc, yst,
            ld, wq_sem, wo_sem, xs_sem, xr_sem, kvs_sem, kvr_sem, fs_sem, as_sem, ar_sem, yl_sem, ys_sem, yr_sem):
    me = lax.axis_index("sp")
    z, c = lax.div(me, 2), lax.rem(me, 2)
    partner = 2 * z + 1 - c
    d = a_s.shape[1]
    half = d // 2
    own = pl.multiple_of(c * T, T)
    oth = pl.multiple_of((1 - c) * T, T)
    col0 = pl.multiple_of(c * half, half)
    col1 = pl.multiple_of((1 - c) * half, half)
    slabs = half // W

    def copy(src, dst, sem):
        return pltpu.make_async_copy(src, dst, sem)

    def remote(src, dst, ssem, rsem, to):
        return pltpu.make_async_remote_copy(src_ref=src, dst_ref=dst, send_sem=ssem, recv_sem=rsem, device_id={"sp": to}, device_id_type=MESH)

    load_x = copy(x_ref, xb.at[pl.ds(own, T)], ld.at[0])
    load_t = copy(tab_ref.at[:, pl.ds(pl.multiple_of(z * C, C), C)], cs, ld.at[1])
    load_k = copy(wk_ref, wk_s, ld.at[2])
    load_v = copy(wv_ref, wv_s, ld.at[3])

    def load_q(i):
        return copy(wq_ref.at[:, pl.ds(pl.multiple_of(col0 + i * W, W), W)], wq_s.at[i], wq_sem.at[i])

    def load_o(p, i):
        return copy(wo_ref.at[pl.ds(col1 if p else col0, half), pl.ds(pl.multiple_of(col0 + i * W, W), W)], wo_s.at[p, i], wo_sem.at[p, i])

    for one in (load_x, load_t, load_k, load_v):
        one.start()
    for i in range(slabs):
        load_q(i).start()

    barrier = pltpu.get_barrier_semaphore()
    pl.semaphore_signal(barrier, inc=1, device_id={"sp": partner}, device_id_type=MESH)

    @pl.when(z > 0)
    def _():
        for o in range(2):
            pl.semaphore_signal(barrier, inc=1, device_id={"sp": 2 * z - 2 + o}, device_id_type=MESH)

    @pl.when(z < Z - 1)
    def _():
        for o in range(2):
            pl.semaphore_signal(barrier, inc=1, device_id={"sp": 2 * z + 2 + o}, device_id_type=MESH)

    edge = (z == 0) | (z == Z - 1)

    @pl.when(edge)
    def _():
        pl.semaphore_wait(barrier, 3)

    @pl.when(jnp.logical_not(edge))
    def _():
        pl.semaphore_wait(barrier, 5)

    load_x.wait()
    send_x = remote(xb.at[pl.ds(own, T)], xb.at[pl.ds(own, T)], xs_sem, xr_sem, partner)
    send_x.start()

    def norm(start):
        gain = g_ref[...].astype(F32)

        def rows(i, _):
            here = pl.ds(pl.multiple_of(start + i * 16, 16), 16)
            wide = xb[here, :].astype(F32)
            scale = lax.rsqrt(jnp.mean(wide * wide, -1, keepdims=True) + 1e-6)
            a_s[here, :] = (wide * scale * gain).astype(BF16)

        lax.fori_loop(0, T // 16, rows, None)

    norm(own)

    load_k.wait()
    load_v.wait()
    load_t.wait()
    mine = a_s[pl.ds(own, T), :]
    k = _dot(mine, wk_s[...]).astype(BF16).astype(F32)
    v = _dot(mine, wv_s[...]).astype(BF16)
    cos, sin = cs[0, pl.ds(own, T), :], cs[1, pl.ds(own, T), :]
    k0, k1 = _turn(k[:, :HEAD], cos, sin), _turn(k[:, HEAD:], cos, sin)
    v0, v1 = v[:, :HEAD], v[:, HEAD:]
    rows_of = lambda t: pl.ds(pl.multiple_of(t * T, T), T)

    @pl.when(c == 0)
    def _():
        kvb[0, rows_of(me), :], kvb[1, rows_of(me), :], kvo[0], kvo[1] = k0, v0, k1, v1

    @pl.when(c == 1)
    def _():
        kvb[0, rows_of(me), :], kvb[1, rows_of(me), :], kvo[0], kvo[1] = k1, v1, k0, v0

    def piece(t):
        return kvb.at[:, rows_of(t)]

    to_pair = remote(kvo, piece(me), kvs_sem.at[0], kvr_sem.at[me], partner)
    to_next = remote(piece(me), piece(me), kvs_sem.at[1], kvr_sem.at[me], 2 * z + 2 + c)
    to_cross = remote(kvo, piece(me), kvs_sem.at[2], kvr_sem.at[me], 2 * z + 3 - c)

    @pl.when(z < Z - 1)
    def _():
        to_next.start()
        to_cross.start()

    to_pair.start()

    def arrived(t):
        remote(piece(t), piece(t), kvs_sem.at[0], kvr_sem.at[t], partner).wait_recv()

    def forward(t):
        return remote(piece(t), piece(t), fs_sem.at[t], kvr_sem.at[t], 2 * z + 2 + c)

    def pass_on(back, which):
        t = 2 * (z - back) + (c if which == 0 else 1 - c)

        @pl.when((z >= back) & (z < Z - 1))
        def _():
            arrived(t)
            forward(t).start()

    def queries(i, start, n):
        here = pl.ds(start, n)
        q = _dot(a_s[here, :], wq_s[i]).astype(BF16).astype(F32)
        cos, sin = cs[0, here, :], cs[1, here, :]
        for h in range(W // HEAD):
            q_s[i * (W // HEAD) + h, here, :] = _turn(q[:, h * HEAD : (h + 1) * HEAD], cos, sin)

    load_q(0).wait()
    queries(0, own, T)
    send_x.wait_recv()
    norm(oth)
    queries(0, oth, T)
    for i in range(slabs):
        load_o(0, i).start()

    def more(i, _):
        load_q(i).wait()
        queries(i, 0, C)
        load_o(1, i - 1).start()

    lax.fori_loop(1, slabs - 1, more, None)
    pass_on(1, 0)
    lax.fori_loop(slabs - 1, slabs, more, None)
    load_o(1, slabs - 1).start()
    pass_on(1, 1)

    e = HEAD**-0.5 * LOG2E
    strip = 2 * C
    strips = QH * C // strip
    ones = jnp.ones((8, C), BF16)

    def block(j, first):
        here = pl.ds(pl.multiple_of(j * C, C), C)
        keys = kvb[0, here, :]
        values = jnp.concatenate([kvb[1, here, :].T, ones], axis=0)

        def scores(s):
            return _dot(keys, q_s[2 * s : 2 * s + 2].reshape(strip, HEAD), 1, 1)

        if first:
            shape = (C, strip)
            seen = lax.rem(lax.broadcasted_iota(jnp.int32, shape, 1), C) >= lax.broadcasted_iota(jnp.int32, shape, 0)
        ahead = scores(0)
        for s in range(strips):
            sc = ahead
            if s + 1 < strips:
                ahead = scores(s + 1)
            at = slice(s * strip, (s + 1) * strip)
            if first:
                sc = jnp.where(seen, sc, HIDDEN)
                top = sc.max(axis=0, keepdims=True)
            else:
                old = top_s[:, at]
                top = jnp.maximum(old, sc.max(axis=0, keepdims=True))
            p = jnp.exp2((sc - top) * e).astype(BF16)
            new = _dot(values, p)
            if first:
                mix_s[:, at] = new
            else:
                mix_s[:, at] = mix_s[:, at] * jnp.exp2((old - top) * e) + new
            top_s[:, at] = top

    arrived(partner)
    block(z, True)
    pass_on(2, 0)

    def earlier(i, _):
        j = z - 1 - i

        @pl.when((z == Z - 1) | (i > 1))
        def _():
            arrived(2 * j)
            arrived(2 * j + 1)

        block(j, False)

        @pl.when(i == 0)
        def _():
            pass_on(2, 1)

    lax.fori_loop(0, z, earlier, None)

    def send_at(n):
        there = pl.ds(n * W, W)
        return remote(at_own.at[:, there], at_par.at[:, there], as_sem.at[n], ar_sem.at[n], partner)

    for s in range(strips):
        at = slice(s * strip, (s + 1) * strip)
        out = (mix_s[:HEAD, at] * (1 / mix_s[HEAD : HEAD + 1, at])).T.astype(BF16)
        for h in range(2):
            at_own[:, (2 * s + h) * HEAD : (2 * s + h + 1) * HEAD] = out[h * C : (h + 1) * C]
        if s % 2:
            send_at(s // 2).start()

    def project(i, _):
        load_o(0, i).wait()
        acc[:, pl.ds(pl.multiple_of(i * W, W), W)] = _dot(at_own[...], wo_s[0, i])

    lax.fori_loop(0, slabs, project, None)
    for n in range(slabs):
        send_at(n).wait_recv()

    def cols(core, i):
        return pl.ds(pl.multiple_of(core * half + i * W, W), W)

    def keep_y(i):
        return copy(yst.at[i, pl.ds(own, T)], y_ref.at[:, cols(c, i)], yl_sem.at[i])

    def send_y(i):
        return remote(yst.at[i, pl.ds(oth, T)], y_ref.at[:, cols(c, i)], ys_sem.at[i], yr_sem.at[i], partner)

    def take_y(i):
        return remote(yst.at[i, pl.ds(oth, T)], y_ref.at[:, cols(1 - c, i)], ys_sem.at[i], yr_sem.at[i], partner)

    def finish(i, _):
        load_o(1, i).wait()
        there = pl.ds(pl.multiple_of(i * W, W), W)
        y = acc[:, there] + _dot(at_par[...], wo_s[1, i])
        yst[i] = (xb[:, cols(c, i)].astype(F32) + y).astype(BF16)
        send_y(i).start()
        keep_y(i).start()

    lax.fori_loop(0, slabs, finish, None)

    send_x.wait_send()
    to_pair.wait_send()

    @pl.when(z < Z - 1)
    def _():
        to_next.wait_send()
        to_cross.wait_send()
        lax.fori_loop(0, 2 * z, lambda t, _: forward(t).wait_send(), None)

    for n in range(slabs):
        send_at(n).wait_send()
        send_y(n).wait_send()
        keep_y(n).wait()
        take_y(n).wait_recv()


def _table(rows):
    half = HEAD // 2
    angle = np.arange(rows, dtype=np.float64)[:, None] * float(THETA) ** (-np.arange(half, dtype=np.float64) / half)
    cos, sin = np.cos(angle), np.sin(angle)
    return np.stack([np.concatenate([cos, cos], 1), np.concatenate([-sin, sin], 1)]).astype(np.float32)


def solution(mesh):
    def step(x, gain, wq, wk, wv, wo):
        d = x.shape[1]
        half = d // 2
        slabs = half // W
        hbm = pl.BlockSpec(memory_space=pl.ANY)
        vm = pltpu.VMEM
        dma = pltpu.SemaphoreType.DMA
        scratch = [
            vm((C, d), BF16), vm((C, d), BF16), vm((d, 2 * HEAD), BF16), vm((d, 2 * HEAD), BF16),
            vm((slabs, d, W), BF16), vm((2, slabs, half, W), BF16), vm((2, C, HEAD), F32), vm((QH, C, HEAD), BF16),
            vm((2, Z * C, HEAD), BF16), vm((2, T, HEAD), BF16), vm((1, QH * C), F32), vm((HEAD + 8, QH * C), F32),
            vm((C, half), BF16), vm((C, half), BF16), vm((C, half), F32), vm((slabs, C, W), BF16),
            dma((4,)), dma((slabs,)), dma((2, slabs)), dma, dma, dma((3,)), dma((2 * Z,)), dma((2 * Z,)),
            dma((slabs,)), dma((slabs,)), dma((slabs,)), dma((slabs,)), dma((slabs,)),
        ]
        return pl.pallas_call(
            _kernel,
            out_shape=jax.ShapeDtypeStruct(x.shape, x.dtype),
            in_specs=[hbm, pl.BlockSpec(memory_space=pltpu.VMEM), hbm, hbm, hbm, hbm, hbm],
            out_specs=hbm,
            scratch_shapes=scratch,
            compiler_params=pltpu.CompilerParams(collective_id=0, has_side_effects=True, vmem_limit_bytes=67_043_328),
            name="layer",
        )(x, gain.reshape(1, d), wq, wk, wv, wo, jnp.asarray(_table(Z * C)))

    tokens, whole = P(("dp", "sp"), None), P(None, None)
    return jax.shard_map(
        step,
        mesh=mesh,
        in_specs=(tokens, P(None), whole, whole, whole, whole),
        out_specs=tokens,
        check_vma=False,
    )
```

```python
import functools
import math

import jax
import jax.numpy as jnp
import numpy as np
from jax import lax
from jax.experimental import pallas as pl
from jax.experimental.pallas import tpu as pltpu
from jax.sharding import PartitionSpec as P

HEAD = 128
THETA = 10000
HIDDEN = -2e30
LOG2E = 1.4426950408889634
MESH = pl.DeviceIdType.MESH
F32, BF16 = jnp.float32, jnp.bfloat16
T = 128
C = 2 * T
W = 512
Z = 4
QH = 16


def _dot(a, b, ca=1, cb=0):
    return lax.dot_general(a, b, (((ca,), (cb,)), ((), ())), preferred_element_type=F32)


def _turn(t, cos, sin):
    return (t * cos + pltpu.roll(t, HEAD // 2, 1) * sin).astype(BF16)


def _kernel(x_ref, g_ref, wq_ref, wk_ref, wv_ref, wo_ref, tab_ref, y_ref,
            xb, a_s, wkv_s, wq_s, wo_s, gs, cs, q_s, kvb, kvo, top_s, mix_s, at_own, at_par, acc, yst,
            ld, wq_sem, wo_sem, xs_sem, xr_sem, kvs_sem, kvr_sem, fs_sem, as_sem, ar_sem, ys_sem, yr_sem):
    me = lax.axis_index("sp")
    z, c = lax.div(me, 2), lax.rem(me, 2)
    partner = 2 * z + 1 - c
    d = a_s.shape[1]
    half = d // 2
    own = pl.multiple_of(c * T, T)
    oth = pl.multiple_of((1 - c) * T, T)
    col0 = pl.multiple_of(c * half, half)
    col1 = pl.multiple_of((1 - c) * half, half)
    slabs = half // W

    def copy(src, dst, sem):
        return pltpu.make_async_copy(src, dst, sem)

    def remote(src, dst, ssem, rsem, to):
        return pltpu.make_async_remote_copy(src_ref=src, dst_ref=dst, send_sem=ssem, recv_sem=rsem, device_id={"sp": to}, device_id_type=MESH)

    load_x = copy(x_ref, xb.at[pl.ds(own, T)], ld.at[0])
    load_t = copy(tab_ref.at[:, pl.ds(pl.multiple_of(z * C, C), C)], cs, ld.at[1])
    load_k = copy(wk_ref, wkv_s.at[:, pl.ds(0, 2 * HEAD)], ld.at[2])
    load_v = copy(wv_ref, wkv_s.at[:, pl.ds(2 * HEAD, 2 * HEAD)], ld.at[3])
    load_g = copy(g_ref, gs, ld.at[4])

    def load_q(i):
        return copy(wq_ref.at[:, pl.ds(pl.multiple_of(col0 + i * W, W), W)], wq_s.at[i], wq_sem.at[i])

    def load_o(p, i):
        return copy(wo_ref.at[pl.ds(col1 if p else col0, half), pl.ds(pl.multiple_of(col0 + i * W, W), W)], wo_s.at[p, i], wo_sem.at[p, i])

    for one in (load_x, load_g, load_k, load_v, load_t):
        one.start()

    barrier = pltpu.get_barrier_semaphore()
    pl.semaphore_signal(barrier, inc=1, device_id={"sp": partner}, device_id_type=MESH)

    @pl.when(z > 0)
    def _():
        for o in range(2):
            pl.semaphore_signal(barrier, inc=1, device_id={"sp": 2 * z - 2 + o}, device_id_type=MESH)

    @pl.when(z < Z - 1)
    def _():
        for o in range(2):
            pl.semaphore_signal(barrier, inc=1, device_id={"sp": 2 * z + 2 + o}, device_id_type=MESH)

    edge = (z == 0) | (z == Z - 1)

    @pl.when(edge)
    def _():
        pl.semaphore_wait(barrier, 3)

    @pl.when(jnp.logical_not(edge))
    def _():
        pl.semaphore_wait(barrier, 5)

    load_x.wait()
    load_g.wait()
    send_x = remote(xb.at[pl.ds(own, T)], xb.at[pl.ds(own, T)], xs_sem, xr_sem, partner)
    send_x.start()

    def norm(start):
        gain = gs[...].astype(F32).reshape(1, d)

        def rows(i, _):
            for r in range(2):
                here = pl.ds(pl.multiple_of(start + (2 * i + r) * 16, 16), 16)
                wide = xb[here, :].astype(F32)
                scale = lax.rsqrt(jnp.mean(wide * wide, -1, keepdims=True) + 1e-6)
                a_s[here, :] = (wide * scale * gain).astype(BF16)

        lax.fori_loop(0, T // 32, rows, None)

    norm(own)

    load_q(0).start()
    load_k.wait()
    load_q(1).start()
    load_v.wait()
    load_t.wait()
    kv = _dot(a_s[pl.ds(own, T), :], wkv_s[...]).astype(BF16)
    k, v = kv[:, : 2 * HEAD].astype(F32), kv[:, 2 * HEAD :]
    cos, sin = cs[0, pl.ds(own, T), :], cs[1, pl.ds(own, T), :]
    k0, k1 = _turn(k[:, :HEAD], cos, sin), _turn(k[:, HEAD:], cos, sin)
    v0, v1 = v[:, :HEAD], v[:, HEAD:]
    rows_of = lambda t: pl.ds(pl.multiple_of(t * T, T), T)

    @pl.when(c == 0)
    def _():
        kvb[0, rows_of(me), :], kvb[1, rows_of(me), :], kvo[0], kvo[1] = k0, v0, k1, v1

    @pl.when(c == 1)
    def _():
        kvb[0, rows_of(me), :], kvb[1, rows_of(me), :], kvo[0], kvo[1] = k1, v1, k0, v0

    def piece(t):
        return kvb.at[:, rows_of(t)]

    to_pair = remote(kvo, piece(me), kvs_sem.at[0], kvr_sem.at[me], partner)
    to_next = remote(piece(me), piece(me), kvs_sem.at[1], kvr_sem.at[me], 2 * z + 2 + c)
    to_cross = remote(kvo, piece(me), kvs_sem.at[2], kvr_sem.at[me], 2 * z + 3 - c)

    @pl.when(z < Z - 1)
    def _():
        to_next.start()
        to_cross.start()

    to_pair.start()

    def arrived(t):
        remote(piece(t), piece(t), kvs_sem.at[0], kvr_sem.at[t], partner).wait_recv()

    def forward(t):
        return remote(piece(t), piece(t), fs_sem.at[t], kvr_sem.at[t], 2 * z + 2 + c)

    def pass_on(back, which):
        t = 2 * (z - back) + (c if which == 0 else 1 - c)

        @pl.when((z >= back) & (z < Z - 1))
        def _():
            arrived(t)
            forward(t).start()

    def raw(i, start, n):
        return _dot(a_s[pl.ds(start, n), :], wq_s[i])

    def queries(q, i, start, n):
        here = pl.ds(start, n)
        q = q.astype(BF16).astype(F32)
        cos, sin = cs[0, here, :], cs[1, here, :]
        for h in range(W // HEAD):
            q_s[i * (W // HEAD) + h, here, :] = _turn(q[:, h * HEAD : (h + 1) * HEAD], cos, sin)

    load_q(2).start()
    load_q(0).wait()
    queries(raw(0, own, T), 0, own, T)
    load_q(3).start()
    send_x.wait_recv()
    norm(oth)
    queries(raw(0, oth, T), 0, oth, T)
    load_q(1).wait()
    queries(raw(1, 0, C), 1, 0, C)
    load_o(0, 0).start()
    load_o(0, 1).start()
    pass_on(1, 0)
    load_q(2).wait()
    queries(raw(2, 0, C), 2, 0, C)
    load_o(0, 2).start()
    load_o(0, 3).start()
    pass_on(1, 1)
    load_q(3).wait()
    queries(raw(3, 0, C), 3, 0, C)
    for i in range(slabs):
        load_o(1, i).start()
    pass_on(2, 0)

    e = HEAD**-0.5 * LOG2E
    strip = 2 * C
    strips = QH * C // strip

    def send_at(n):
        there = pl.ds(n * W, W)
        return remote(at_own.at[:, there], at_par.at[:, there], as_sem.at[n], ar_sem.at[n], partner)

    def finish_heads(s, mix):
        out = (mix[:HEAD] * (1 / mix[HEAD : HEAD + 1])).T.astype(BF16)
        for h in range(2):
            at_own[:, (2 * s + h) * HEAD : (2 * s + h + 1) * HEAD] = out[h * C : (h + 1) * C]
        if s % 2:
            send_at(s // 2).start()

    def block(j, n, ahead, first, last):
        size = n * C
        here = pl.ds(pl.multiple_of(j * C, C), size)
        keys = kvb[0, here, :]
        values = jnp.concatenate([kvb[1, here, :].T, jnp.ones((8, size), BF16)], axis=0)
        waiting = []

        def scores(s):
            if s < strips:
                waiting.append(_dot(keys, q_s[2 * s : 2 * s + 2].reshape(strip, HEAD), 1, 1))

        if first:
            shape = (C, strip)
            seen = lax.rem(lax.broadcasted_iota(jnp.int32, shape, 1), C) >= lax.broadcasted_iota(jnp.int32, shape, 0)
        for s in range(ahead):
            scores(s)
        for s in range(strips):
            scores(s + ahead)
            sc = waiting.pop(0)
            at = slice(s * strip, (s + 1) * strip)
            if first:
                low = jnp.where(seen, sc[size - C :], HIDDEN)
                sc = low if n == 1 else jnp.concatenate([sc[: size - C], low], axis=0)
                top = sc.max(axis=0, keepdims=True)
            else:
                old = top_s[:, at]
                top = jnp.maximum(old, sc.max(axis=0, keepdims=True))
            mix = _dot(values, jnp.exp2((sc - top) * e).astype(BF16))
            if not first:
                mix = mix_s[:, at] * jnp.exp2((old - top) * e) + mix
            if last:
                finish_heads(s, mix)
            else:
                mix_s[:, at] = mix
                top_s[:, at] = top

    arrived(partner)

    @pl.when(z == 0)
    def _():
        block(z, 1, 2, True, False)

    @pl.when(z > 0)
    def _():
        @pl.when(z == Z - 1)
        def _():
            arrived(2 * z - 2)
            arrived(2 * z - 1)

        block(z - 1, 2, 1, True, False)

    pass_on(2, 1)

    @pl.when(z == Z - 1)
    def _():
        arrived(2 * z - 4)
        arrived(2 * z - 3)
        block(z - 2, 1, 3, False, False)
        arrived(0)
        arrived(1)

    @pl.when(z > 1)
    def _():
        block(0, 1, 3, False, True)

    @pl.when(z < 2)
    def _():
        for s in range(strips):
            finish_heads(s, mix_s[:, s * strip : (s + 1) * strip])

    for i in range(slabs):
        load_o(0, i).wait()
        acc[:, i * W : (i + 1) * W] = _dot(at_own[...], wo_s[0, i])
    for n in range(slabs):
        send_at(n).wait_recv()

    def cols(core, i):
        return pl.ds(pl.multiple_of(core * half + i * W, W), W)

    def send_y(i):
        return remote(yst.at[i], y_ref.at[:, cols(c, i)], ys_sem.at[i], yr_sem.at[i], partner)

    def take_y(i):
        return remote(yst.at[i], y_ref.at[:, cols(1 - c, i)], ys_sem.at[i], yr_sem.at[i], partner)

    for i in range(slabs):
        load_o(1, i).wait()
        for start, where in ((oth, yst.at[i]), (own, y_ref.at[:, cols(c, i)])):
            here = pl.ds(start, T)
            y = acc[here, i * W : (i + 1) * W] + _dot(at_par[here, :], wo_s[1, i])
            where[...] = (xb[here, cols(c, i)].astype(F32) + y).astype(BF16)
            if start is oth:
                send_y(i).start()

    send_x.wait_send()
    to_pair.wait_send()

    @pl.when(z < Z - 1)
    def _():
        to_next.wait_send()
        to_cross.wait_send()
        lax.fori_loop(0, 2 * z, lambda t, _: forward(t).wait_send(), None)

    for n in range(slabs):
        send_at(n).wait_send()
        send_y(n).wait_send()
        take_y(n).wait_recv()


def _table(rows):
    half = HEAD // 2
    angle = np.arange(rows, dtype=np.float64)[:, None] * float(THETA) ** (-np.arange(half, dtype=np.float64) / half)
    cos, sin = np.cos(angle), np.sin(angle)
    return np.stack([np.concatenate([cos, cos], 1), np.concatenate([-sin, sin], 1)]).astype(np.float32)


def solution(mesh):
    def step(x, gain, wq, wk, wv, wo):
        d = x.shape[1]
        half = d // 2
        slabs = half // W
        hbm = pl.BlockSpec(memory_space=pl.ANY)
        vm = pltpu.VMEM
        dma = pltpu.SemaphoreType.DMA
        scratch = [
            vm((C, d), BF16), vm((C, d), BF16), vm((d, 4 * HEAD), BF16),
            vm((slabs, d, W), BF16), vm((2, slabs, half, W), BF16), vm((d,), BF16), vm((2, C, HEAD), F32), vm((QH, C, HEAD), BF16),
            vm((2, Z * C, HEAD), BF16), vm((2, T, HEAD), BF16), vm((1, QH * C), F32), vm((HEAD + 8, QH * C), F32),
            vm((C, half), BF16), vm((C, half), BF16), vm((C, half), F32), vm((slabs, T, W), BF16),
            dma((5,)), dma((slabs,)), dma((2, slabs)), dma, dma, dma((3,)), dma((2 * Z,)), dma((2 * Z,)),
            dma((slabs,)), dma((slabs,)), dma((slabs,)), dma((slabs,)),
        ]
        return pl.pallas_call(
            _kernel,
            out_shape=jax.ShapeDtypeStruct(x.shape, x.dtype),
            in_specs=[hbm] * 7,
            out_specs=pl.BlockSpec(memory_space=pltpu.VMEM),
            scratch_shapes=scratch,
            compiler_params=pltpu.CompilerParams(collective_id=0, has_side_effects=True, vmem_limit_bytes=60 * 2**20),
            name="layer",
        )(x, gain, wq, wk, wv, wo, jnp.asarray(_table(Z * C)))

    tokens, whole = P(("dp", "sp"), None), P(None, None)
    return jax.shard_map(
        step,
        mesh=mesh,
        in_specs=(tokens, P(None), whole, whole, whole, whole),
        out_specs=tokens,
        check_vma=False,
    )
```

```python
import functools
import math

import jax
import jax.numpy as jnp
import numpy as np
from jax import lax
from jax.experimental import pallas as pl
from jax.experimental.pallas import tpu as pltpu
from jax.sharding import PartitionSpec as P

HEAD = 128
THETA = 10000
HIDDEN = -2e30
LOG2E = 1.4426950408889634
MESH = pl.DeviceIdType.MESH
F32, BF16 = jnp.float32, jnp.bfloat16
T = 128
C = 2 * T
W = 512
Z = 4
QH = 16


def _dot(a, b, ca=1, cb=0):
    return lax.dot_general(a, b, (((ca,), (cb,)), ((), ())), preferred_element_type=F32)


def _turn(t, cos, sin):
    return (t * cos + pltpu.roll(t, HEAD // 2, 1) * sin).astype(BF16)


def _kernel(x_ref, g_ref, wq_ref, wk_ref, wv_ref, wo_ref, tab_ref, y_ref,
            xb, a_s, wkv_s, wq_s, wo_s, gs, cs, q_s, kvb, kvo, top_s, mix_s, at_own, at_par, acc, yst,
            ld, wq_sem, wo_sem, xs_sem, xr_sem, kvs_sem, kvr_sem, fs_sem, as_sem, ar_sem, ys_sem, yr_sem):
    me = lax.axis_index("sp")
    z, c = lax.div(me, 2), lax.rem(me, 2)
    partner = 2 * z + 1 - c
    d = a_s.shape[1]
    half = d // 2
    own = pl.multiple_of(c * T, T)
    oth = pl.multiple_of((1 - c) * T, T)
    col0 = pl.multiple_of(c * half, half)
    col1 = pl.multiple_of((1 - c) * half, half)
    slabs = half // W

    def copy(src, dst, sem):
        return pltpu.make_async_copy(src, dst, sem)

    def remote(src, dst, ssem, rsem, to):
        return pltpu.make_async_remote_copy(src_ref=src, dst_ref=dst, send_sem=ssem, recv_sem=rsem, device_id={"sp": to}, device_id_type=MESH)

    load_x = copy(x_ref, xb.at[pl.ds(own, T)], ld.at[0])
    load_t = copy(tab_ref.at[:, pl.ds(pl.multiple_of(z * C, C), C)], cs, ld.at[1])
    load_k = copy(wk_ref, wkv_s.at[:, pl.ds(0, 2 * HEAD)], ld.at[2])
    load_v = copy(wv_ref, wkv_s.at[:, pl.ds(2 * HEAD, 2 * HEAD)], ld.at[3])
    load_g = copy(g_ref, gs, ld.at[4])

    def load_q(i):
        return copy(wq_ref.at[:, pl.ds(pl.multiple_of(col0 + i * W, W), W)], wq_s.at[i], wq_sem.at[i])

    def load_o(p, i):
        return copy(wo_ref.at[pl.ds(col1 if p else col0, half), pl.ds(pl.multiple_of(col0 + i * W, W), W)], wo_s.at[p, i], wo_sem.at[p, i])

    for one in (load_x, load_g, load_k, load_v, load_t):
        one.start()

    barrier = pltpu.get_barrier_semaphore()
    pl.semaphore_signal(barrier, inc=1, device_id={"sp": partner}, device_id_type=MESH)

    @pl.when(z > 0)
    def _():
        for o in range(2):
            pl.semaphore_signal(barrier, inc=1, device_id={"sp": 2 * z - 2 + o}, device_id_type=MESH)

    @pl.when(z < Z - 1)
    def _():
        for o in range(2):
            pl.semaphore_signal(barrier, inc=1, device_id={"sp": 2 * z + 2 + o}, device_id_type=MESH)

    edge = (z == 0) | (z == Z - 1)

    @pl.when(edge)
    def _():
        pl.semaphore_wait(barrier, 3)

    @pl.when(jnp.logical_not(edge))
    def _():
        pl.semaphore_wait(barrier, 5)

    load_x.wait()
    load_g.wait()
    send_x = remote(xb.at[pl.ds(own, T)], xb.at[pl.ds(own, T)], xs_sem, xr_sem, partner)
    send_x.start()

    def norm(start):
        gain = gs[...].astype(F32).reshape(1, d)

        def rows(i, _):
            for r in range(2):
                here = pl.ds(pl.multiple_of(start + (2 * i + r) * 16, 16), 16)
                wide = xb[here, :].astype(F32)
                scale = lax.rsqrt(jnp.mean(wide * wide, -1, keepdims=True) + 1e-6)
                a_s[here, :] = (wide * scale * gain).astype(BF16)

        lax.fori_loop(0, T // 32, rows, None)

    norm(own)

    load_q(0).start()
    load_k.wait()
    load_q(1).start()
    load_v.wait()
    load_t.wait()
    kv = _dot(a_s[pl.ds(own, T), :], wkv_s[...]).astype(BF16)
    k, v = kv[:, : 2 * HEAD].astype(F32), kv[:, 2 * HEAD :]
    cos, sin = cs[0, pl.ds(own, T), :], cs[1, pl.ds(own, T), :]
    k0, k1 = _turn(k[:, :HEAD], cos, sin), _turn(k[:, HEAD:], cos, sin)
    v0, v1 = v[:, :HEAD], v[:, HEAD:]
    rows_of = lambda t: pl.ds(pl.multiple_of(t * T, T), T)

    @pl.when(c == 0)
    def _():
        kvb[0, rows_of(me), :], kvb[1, rows_of(me), :], kvo[0], kvo[1] = k0, v0, k1, v1

    @pl.when(c == 1)
    def _():
        kvb[0, rows_of(me), :], kvb[1, rows_of(me), :], kvo[0], kvo[1] = k1, v1, k0, v0

    def piece(t):
        return kvb.at[:, rows_of(t)]

    to_pair = remote(kvo, piece(me), kvs_sem.at[0], kvr_sem.at[me], partner)
    to_next = remote(piece(me), piece(me), kvs_sem.at[1], kvr_sem.at[me], 2 * z + 2 + c)
    to_cross = remote(kvo, piece(me), kvs_sem.at[2], kvr_sem.at[me], 2 * z + 3 - c)

    @pl.when(z < Z - 1)
    def _():
        to_next.start()
        to_cross.start()

    to_pair.start()

    def arrived(t):
        remote(piece(t), piece(t), kvs_sem.at[0], kvr_sem.at[t], partner).wait_recv()

    def forward(t):
        return remote(piece(t), piece(t), fs_sem.at[t], kvr_sem.at[t], 2 * z + 2 + c)

    def pass_on(back, which):
        t = 2 * (z - back) + (c if which == 0 else 1 - c)

        @pl.when((z >= back) & (z < Z - 1))
        def _():
            arrived(t)
            forward(t).start()

    def raw(i, start, n):
        return _dot(a_s[pl.ds(start, n), :], wq_s[i])

    def queries(q, i, start, n):
        here = pl.ds(start, n)
        q = q.astype(BF16).astype(F32)
        cos, sin = cs[0, here, :], cs[1, here, :]
        for h in range(W // HEAD):
            q_s[i * (W // HEAD) + h, here, :] = _turn(q[:, h * HEAD : (h + 1) * HEAD], cos, sin)

    load_q(2).start()
    load_q(0).wait()
    queries(raw(0, own, T), 0, own, T)
    load_q(3).start()
    send_x.wait_recv()
    norm(oth)
    queries(raw(0, oth, T), 0, oth, T)
    load_q(1).wait()
    queries(raw(1, 0, C), 1, 0, C)
    load_o(0, 0).start()
    load_o(0, 1).start()
    pass_on(1, 0)
    load_q(2).wait()
    queries(raw(2, 0, C), 2, 0, C)
    load_o(0, 2).start()
    load_o(0, 3).start()
    pass_on(1, 1)
    load_q(3).wait()
    queries(raw(3, 0, C), 3, 0, C)
    for i in range(slabs):
        load_o(1, i).start()
    pass_on(2, 0)

    e = HEAD**-0.5 * LOG2E
    strip = 2 * C
    strips = QH * C // strip

    def send_at(n):
        there = pl.ds(n * W, W)
        return remote(at_own.at[:, there], at_par.at[:, there], as_sem.at[n], ar_sem.at[n], partner)

    def finish_heads(s, mix):
        out = (mix[:HEAD] * (1 / mix[HEAD : HEAD + 1])).T.astype(BF16)
        for h in range(2):
            at_own[:, (2 * s + h) * HEAD : (2 * s + h + 1) * HEAD] = out[h * C : (h + 1) * C]
        if s % 2:
            send_at(s // 2).start()

    def block(j, n, ahead, first, last):
        size = n * C
        here = pl.ds(pl.multiple_of(j * C, C), size)
        keys = kvb[0, here, :]
        values = jnp.concatenate([kvb[1, here, :].T, jnp.ones((8, size), BF16)], axis=0)
        waiting = []

        def scores(s):
            if s < strips:
                waiting.append(_dot(keys, q_s[2 * s : 2 * s + 2].reshape(strip, HEAD), 1, 1))

        if first:
            shape = (C, strip)
            seen = lax.rem(lax.broadcasted_iota(jnp.int32, shape, 1), C) >= lax.broadcasted_iota(jnp.int32, shape, 0)
        for s in range(ahead):
            scores(s)
        for s in range(strips):
            scores(s + ahead)
            sc = waiting.pop(0)
            at = slice(s * strip, (s + 1) * strip)
            if first:
                low = jnp.where(seen, sc[size - C :], HIDDEN)
                sc = low if n == 1 else jnp.concatenate([sc[: size - C], low], axis=0)
                top = sc.max(axis=0, keepdims=True)
            else:
                old = top_s[:, at]
                top = jnp.maximum(old, sc.max(axis=0, keepdims=True))
            mix = _dot(values, jnp.exp2((sc - top) * e).astype(BF16))
            if not first:
                mix = mix_s[:, at] * jnp.exp2((old - top) * e) + mix
            if last:
                finish_heads(s, mix)
            else:
                mix_s[:, at] = mix
                top_s[:, at] = top

    arrived(partner)

    @pl.when(z == 0)
    def _():
        block(z, 1, 2, True, False)

    @pl.when(z > 0)
    def _():
        @pl.when(z == Z - 1)
        def _():
            arrived(2 * z - 2)
            arrived(2 * z - 1)

        block(z - 1, 2, 1, True, False)

    pass_on(2, 1)

    @pl.when(z == Z - 1)
    def _():
        arrived(2 * z - 4)
        arrived(2 * z - 3)
        block(z - 2, 1, 3, False, False)
        arrived(0)
        arrived(1)

    @pl.when(z > 1)
    def _():
        block(0, 1, 3, False, True)

    @pl.when(z < 2)
    def _():
        for s in range(strips):
            finish_heads(s, mix_s[:, s * strip : (s + 1) * strip])

    for i in range(slabs):
        load_o(0, i).wait()
        acc[:, i * W : (i + 1) * W] = _dot(at_own[...], wo_s[0, i])
    for n in range(slabs):
        send_at(n).wait_recv()

    def cols(core, i):
        return pl.ds(pl.multiple_of(core * half + i * W, W), W)

    def send_y(i):
        return remote(yst.at[i], y_ref.at[:, cols(c, i)], ys_sem.at[i], yr_sem.at[i], partner)

    def take_y(i):
        return remote(yst.at[i], y_ref.at[:, cols(1 - c, i)], ys_sem.at[i], yr_sem.at[i], partner)

    for i in range(slabs):
        load_o(1, i).wait()
        for start, where in ((oth, yst.at[i]), (own, y_ref.at[:, cols(c, i)])):
            here = pl.ds(start, T)
            y = acc[here, i * W : (i + 1) * W] + _dot(at_par[here, :], wo_s[1, i])
            where[...] = (xb[here, cols(c, i)].astype(F32) + y).astype(BF16)
            if start is oth:
                send_y(i).start()

    send_x.wait_send()
    to_pair.wait_send()

    @pl.when(z < Z - 1)
    def _():
        to_next.wait_send()
        to_cross.wait_send()
        lax.fori_loop(0, 2 * z, lambda t, _: forward(t).wait_send(), None)

    for n in range(slabs):
        send_at(n).wait_send()
        send_y(n).wait_send()
        take_y(n).wait_recv()


def _table(rows):
    half = HEAD // 2
    angle = np.arange(rows, dtype=np.float64)[:, None] * float(THETA) ** (-np.arange(half, dtype=np.float64) / half)
    cos, sin = np.cos(angle), np.sin(angle)
    return np.stack([np.concatenate([cos, cos], 1), np.concatenate([-sin, sin], 1)]).astype(np.float32)


def solution(mesh):
    def step(x, gain, wq, wk, wv, wo):
        d = x.shape[1]
        half = d // 2
        slabs = half // W
        hbm = pl.BlockSpec(memory_space=pl.ANY)
        vm = pltpu.VMEM
        dma = pltpu.SemaphoreType.DMA
        scratch = [
            vm((C, d), BF16), vm((C, d), BF16), vm((d, 4 * HEAD), BF16),
            vm((slabs, d, W), BF16), vm((2, slabs, half, W), BF16), vm((d,), BF16), vm((2, C, HEAD), F32), vm((QH, C, HEAD), BF16),
            vm((2, Z * C, HEAD), BF16), vm((2, T, HEAD), BF16), vm((1, QH * C), F32), vm((HEAD + 8, QH * C), F32),
            vm((C, half), BF16), vm((C, half), BF16), vm((C, half), F32), vm((slabs, T, W), BF16),
            dma((5,)), dma((slabs,)), dma((2, slabs)), dma, dma, dma((3,)), dma((2 * Z,)), dma((2 * Z,)),
            dma((slabs,)), dma((slabs,)), dma((slabs,)), dma((slabs,)),
        ]
        return pl.pallas_call(
            _kernel,
            out_shape=pltpu.VMEM(x.shape, x.dtype),
            in_specs=[hbm] * 7,
            out_specs=pl.BlockSpec(memory_space=pltpu.VMEM),
            scratch_shapes=scratch,
            compiler_params=pltpu.CompilerParams(collective_id=0, has_side_effects=True, vmem_limit_bytes=60 * 2**20),
            name="layer",
        )(x, gain, wq, wk, wv, wo, jnp.asarray(_table(Z * C)))

    tokens, whole = P(("dp", "sp"), None), P(None, None)
    return jax.shard_map(
        step,
        mesh=mesh,
        in_specs=(tokens, P(None), whole, whole, whole, whole),
        out_specs=tokens,
        check_vma=False,
    )
```

```python
import functools
import math

import jax
import jax.numpy as jnp
import numpy as np
from jax import lax
from jax.experimental import pallas as pl
from jax.experimental.pallas import tpu as pltpu
from jax.sharding import PartitionSpec as P

HEAD = 128
THETA = 10000
HIDDEN = -2e30
LOG2E = 1.4426950408889634
MESH = pl.DeviceIdType.MESH
F32, BF16 = jnp.float32, jnp.bfloat16
T = 128
C = 2 * T
W = 512
Z = 4
QH = 16


def _dot(a, b, ca=1, cb=0):
    return lax.dot_general(a, b, (((ca,), (cb,)), ((), ())), preferred_element_type=F32)


def _turn(t, cos, sin):
    return (t * cos + pltpu.roll(t, HEAD // 2, 1) * sin).astype(BF16)


def _kernel(x_ref, g_ref, wq_ref, wk_ref, wv_ref, wo_ref, tab_ref, y_ref,
            xb, a_s, wkv_s, wq_s, wo_s, gs, cs, q_s, kvb, kvo, top_s, mix_s, at_own, at_par, acc, yst,
            ld, kv_sem, wq_sem, wo_sem, xs_sem, xr_sem, kvs_sem, kvr_sem, fs_sem, as_sem, ar_sem, ys_sem, yr_sem):
    me = lax.axis_index("sp")
    z, c = lax.div(me, 2), lax.rem(me, 2)
    partner = 2 * z + 1 - c
    d = a_s.shape[1]
    half = d // 2
    own = pl.multiple_of(c * T, T)
    oth = pl.multiple_of((1 - c) * T, T)
    col0 = pl.multiple_of(c * half, half)
    col1 = pl.multiple_of((1 - c) * half, half)
    slabs = half // W

    def copy(src, dst, sem):
        return pltpu.make_async_copy(src, dst, sem)

    def remote(src, dst, ssem, rsem, to):
        return pltpu.make_async_remote_copy(src_ref=src, dst_ref=dst, send_sem=ssem, recv_sem=rsem, device_id={"sp": to}, device_id_type=MESH)

    load_x = copy(x_ref, xb.at[pl.ds(own, T)], ld.at[0])
    load_t = copy(tab_ref.at[:, pl.ds(pl.multiple_of(z * C, C), C)], cs, ld.at[1])
    load_g = copy(g_ref, gs, ld.at[2])

    def load_kv(n):
        rows = pl.ds(n * half, half)
        return [copy(w.at[rows], wkv_s.at[rows, pl.ds(i * 2 * HEAD, 2 * HEAD)], kv_sem.at[n, i]) for i, w in enumerate((wk_ref, wv_ref))]

    def load_q(i):
        return copy(wq_ref.at[:, pl.ds(pl.multiple_of(col0 + i * W, W), W)], wq_s.at[i], wq_sem.at[i])

    def load_o(p, i):
        return copy(wo_ref.at[pl.ds(col1 if p else col0, half), pl.ds(pl.multiple_of(col0 + i * W, W), W)], wo_s.at[p, i], wo_sem.at[p, i])

    for one in (load_x, load_g, *load_kv(0), *load_kv(1), load_t):
        one.start()

    barrier = pltpu.get_barrier_semaphore()
    pl.semaphore_signal(barrier, inc=1, device_id={"sp": partner}, device_id_type=MESH)

    for o in range(2):
        for side in (1, Z - 1):
            pl.semaphore_signal(barrier, inc=1, device_id={"sp": 2 * lax.rem(z + side, Z) + o}, device_id_type=MESH)

    pl.semaphore_wait(barrier, 5)
    load_x.wait()
    load_g.wait()
    send_x = remote(xb.at[pl.ds(own, T)], xb.at[pl.ds(own, T)], xs_sem, xr_sem, partner)
    send_x.start()
    load_q(0).start()

    def norm(start):
        gain = gs[...].astype(F32).reshape(1, d)

        def rows(i, _):
            for r in range(2):
                here = pl.ds(pl.multiple_of(start + (2 * i + r) * 16, 16), 16)
                wide = xb[here, :].astype(F32)
                scale = lax.rsqrt(jnp.mean(wide * wide, -1, keepdims=True) + 1e-6)
                a_s[here, :] = (wide * scale * gain).astype(BF16)

        lax.fori_loop(0, T // 32, rows, None)

    norm(own)

    mine = a_s[pl.ds(own, T), :]
    for one in load_kv(0):
        one.wait()
    kv = _dot(mine[:, :half], wkv_s[:half])
    for one in load_kv(1):
        one.wait()
    load_t.wait()
    load_q(1).start()
    kv = (kv + _dot(mine[:, half:], wkv_s[half:])).astype(BF16)
    k, v = kv[:, : 2 * HEAD].astype(F32), kv[:, 2 * HEAD :]
    cos, sin = cs[0, pl.ds(own, T), :], cs[1, pl.ds(own, T), :]
    k0, k1 = _turn(k[:, :HEAD], cos, sin), _turn(k[:, HEAD:], cos, sin)
    v0, v1 = v[:, :HEAD], v[:, HEAD:]
    rows_of = lambda t: pl.ds(pl.multiple_of(t * T, T), T)

    @pl.when(c == 0)
    def _():
        kvb[0, rows_of(me), :], kvb[1, rows_of(me), :], kvo[0], kvo[1] = k0, v0, k1, v1

    @pl.when(c == 1)
    def _():
        kvb[0, rows_of(me), :], kvb[1, rows_of(me), :], kvo[0], kvo[1] = k1, v1, k0, v0

    def piece(t):
        return kvb.at[:, rows_of(t)]

    to_pair = remote(kvo, piece(me), kvs_sem.at[0], kvr_sem.at[me], partner)
    to_next = remote(piece(me), piece(me), kvs_sem.at[1], kvr_sem.at[me], 2 * z + 2 + c)
    to_cross = remote(kvo, piece(me), kvs_sem.at[2], kvr_sem.at[me], 2 * z + 3 - c)

    @pl.when(z < Z - 1)
    def _():
        to_next.start()
        to_cross.start()

    to_pair.start()

    def far(o):
        return remote(kvo if o else piece(me), piece(me), kvs_sem.at[3 + o], kvr_sem.at[me], 2 * (Z - 1) + (1 - c if o else c))

    def arrived(t):
        remote(piece(t), piece(t), kvs_sem.at[0], kvr_sem.at[t], partner).wait_recv()

    def forward(t):
        return remote(piece(t), piece(t), fs_sem.at[t], kvr_sem.at[t], 2 * z + 2 + c)

    def pass_on(which):
        t = 2 * z - 2 + (c if which == 0 else 1 - c)

        @pl.when((z > 0) & (z < Z - 1))
        def _():
            arrived(t)
            forward(t).start()

    def raw(i, start, n):
        return _dot(a_s[pl.ds(start, n), :], wq_s[i])

    def queries(q, i, start, n):
        here = pl.ds(start, n)
        q = q.astype(BF16).astype(F32)
        cos, sin = cs[0, here, :], cs[1, here, :]
        for h in range(W // HEAD):
            q_s[i * (W // HEAD) + h, here, :] = _turn(q[:, h * HEAD : (h + 1) * HEAD], cos, sin)

    load_q(2).start()
    load_q(0).wait()
    queries(raw(0, own, T), 0, own, T)
    load_q(3).start()
    send_x.wait_recv()
    norm(oth)

    @pl.when(z == 0)
    def _():
        far(0).start()
        far(1).start()

    load_q(1).wait()
    q0, q1 = raw(0, oth, T), raw(1, 0, C)
    queries(q0, 0, oth, T)
    queries(q1, 1, 0, C)
    load_o(0, 0).start()
    load_o(0, 1).start()
    pass_on(0)
    load_q(2).wait()
    queries(raw(2, 0, C), 2, 0, C)
    load_o(0, 2).start()
    load_o(0, 3).start()
    pass_on(1)
    load_q(3).wait()
    queries(raw(3, 0, C), 3, 0, C)
    for i in range(slabs):
        load_o(1, i).start()

    e = HEAD**-0.5 * LOG2E
    strip = 2 * C
    strips = QH * C // strip

    def send_at(n):
        there = pl.ds(n * W, W)
        return remote(at_own.at[:, there], at_par.at[:, there], as_sem.at[n], ar_sem.at[n], partner)

    def finish_heads(s, mix):
        out = (mix[:HEAD] * (1 / mix[HEAD : HEAD + 1])).T.astype(BF16)
        for h in range(2):
            at_own[:, (2 * s + h) * HEAD : (2 * s + h + 1) * HEAD] = out[h * C : (h + 1) * C]
        if s % 2:
            send_at(s // 2).start()

    def block(j, n, ahead, first, last):
        size = n * C
        here = pl.ds(pl.multiple_of(j * C, C), size)
        keys = kvb[0, here, :]
        values = jnp.concatenate([kvb[1, here, :].T, jnp.ones((8, size), BF16)], axis=0)
        waiting = []

        def scores(s):
            if s < strips:
                waiting.append(_dot(keys, q_s[2 * s : 2 * s + 2].reshape(strip, HEAD), 1, 1))

        if first:
            shape = (C, strip)
            seen = lax.rem(lax.broadcasted_iota(jnp.int32, shape, 1), C) >= lax.broadcasted_iota(jnp.int32, shape, 0)
        for s in range(ahead):
            scores(s)
        for s in range(strips):
            scores(s + ahead)
            sc = waiting.pop(0)
            at = slice(s * strip, (s + 1) * strip)
            if first:
                low = jnp.where(seen, sc[size - C :], HIDDEN)
                sc = low if n == 1 else jnp.concatenate([sc[: size - C], low], axis=0)
                top = sc.max(axis=0, keepdims=True)
            else:
                old = top_s[:, at]
                top = jnp.maximum(old, sc.max(axis=0, keepdims=True))
            mix = _dot(values, jnp.exp2((sc - top) * e).astype(BF16))
            if not first:
                mix = mix_s[:, at] * jnp.exp2((old - top) * e) + mix
            if last:
                finish_heads(s, mix)
            else:
                mix_s[:, at] = mix
                top_s[:, at] = top

    arrived(partner)

    @pl.when(z == 0)
    def _():
        block(z, 1, 3, True, False)

    @pl.when(z > 0)
    def _():
        @pl.when(z == Z - 1)
        def _():
            arrived(2 * z - 2)
            arrived(2 * z - 1)

        block(z - 1, 2, 3, True, False)

    @pl.when(z == Z - 1)
    def _():
        arrived(2 * z - 4)
        arrived(2 * z - 3)
        block(z - 2, 1, 3, False, False)

    @pl.when(z > 1)
    def _():
        arrived(0)
        arrived(1)
        block(0, 1, 3, False, True)

    @pl.when(z < 2)
    def _():
        for s in range(strips):
            finish_heads(s, mix_s[:, s * strip : (s + 1) * strip])

    for p in range(2):
        for i in range(slabs):
            load_o(p, i).wait()
    for i in range(slabs):
        acc[:, i * W : (i + 1) * W] = _dot(at_own[...], wo_s[0, i])
    for n in range(slabs):
        send_at(n).wait_recv()

    def cols(core, i):
        return pl.ds(pl.multiple_of(core * half + i * W, W), W)

    def send_y(i):
        return remote(yst.at[i], y_ref.at[:, cols(c, i)], ys_sem.at[i], yr_sem.at[i], partner)

    def take_y(i):
        return remote(yst.at[i], y_ref.at[:, cols(1 - c, i)], ys_sem.at[i], yr_sem.at[i], partner)

    for i in range(slabs):
        y = acc[:, i * W : (i + 1) * W] + _dot(at_par[...], wo_s[1, i])
        acc[:, i * W : (i + 1) * W] = xb[:, cols(c, i)].astype(F32) + y
        yst[i] = acc[pl.ds(oth, T), i * W : (i + 1) * W].astype(BF16)
        send_y(i).start()
        y_ref[:, cols(c, i)] = acc[pl.ds(own, T), i * W : (i + 1) * W].astype(BF16)

    send_x.wait_send()
    to_pair.wait_send()

    @pl.when(z < Z - 1)
    def _():
        to_next.wait_send()
        to_cross.wait_send()

    @pl.when((z > 0) & (z < Z - 1))
    def _():
        forward(2 * z - 2).wait_send()
        forward(2 * z - 1).wait_send()

    @pl.when(z == 0)
    def _():
        far(0).wait_send()
        far(1).wait_send()

    for n in range(slabs):
        send_at(n).wait_send()
        send_y(n).wait_send()
        take_y(n).wait_recv()


def _table(rows):
    half = HEAD // 2
    angle = np.arange(rows, dtype=np.float64)[:, None] * float(THETA) ** (-np.arange(half, dtype=np.float64) / half)
    cos, sin = np.cos(angle), np.sin(angle)
    return np.stack([np.concatenate([cos, cos], 1), np.concatenate([-sin, sin], 1)]).astype(np.float32)


def solution(mesh):
    def step(x, gain, wq, wk, wv, wo):
        d = x.shape[1]
        half = d // 2
        slabs = half // W
        hbm = pl.BlockSpec(memory_space=pl.ANY)
        vm = pltpu.VMEM
        dma = pltpu.SemaphoreType.DMA
        scratch = [
            vm((C, d), BF16), vm((C, d), BF16), vm((d, 4 * HEAD), BF16),
            vm((slabs, d, W), BF16), vm((2, slabs, half, W), BF16), vm((d,), BF16), vm((2, C, HEAD), F32), vm((QH, C, HEAD), BF16),
            vm((2, Z * C, HEAD), BF16), vm((2, T, HEAD), BF16), vm((1, QH * C), F32), vm((HEAD + 8, QH * C), F32),
            vm((C, half), BF16), vm((C, half), BF16), vm((C, half), F32), vm((slabs, T, W), BF16),
            dma((3,)), dma((2, 2)), dma((slabs,)), dma((2, slabs)), dma, dma, dma((5,)), dma((2 * Z,)), dma((2 * Z,)),
            dma((slabs,)), dma((slabs,)), dma((slabs,)), dma((slabs,)),
        ]
        return pl.pallas_call(
            _kernel,
            out_shape=pltpu.VMEM(x.shape, x.dtype),
            in_specs=[hbm] * 7,
            out_specs=pl.BlockSpec(memory_space=pltpu.VMEM),
            scratch_shapes=scratch,
            compiler_params=pltpu.CompilerParams(collective_id=0, has_side_effects=True, vmem_limit_bytes=60 * 2**20),
            name="layer",
        )(x, gain, wq, wk, wv, wo, jnp.asarray(_table(Z * C)))

    tokens, whole = P(("dp", "sp"), None), P(None, None)
    return jax.shard_map(
        step,
        mesh=mesh,
        in_specs=(tokens, P(None), whole, whole, whole, whole),
        out_specs=tokens,
        check_vma=False,
    )
```

```python
import functools
import math

import jax
import jax.numpy as jnp
import numpy as np
from jax import lax
from jax.experimental import pallas as pl
from jax.experimental.pallas import tpu as pltpu
from jax.sharding import PartitionSpec as P

HEAD = 128
THETA = 10000
HIDDEN = -2e30
LOG2E = 1.4426950408889634
MESH = pl.DeviceIdType.MESH
F32, BF16 = jnp.float32, jnp.bfloat16
T = 128
C = 2 * T
W = 512
Z = 4
QH = 16


def _dot(a, b, ca=1, cb=0):
    return lax.dot_general(a, b, (((ca,), (cb,)), ((), ())), preferred_element_type=F32)


def _turn(t, cos, sin):
    return (t * cos + pltpu.roll(t, HEAD // 2, 1) * sin).astype(BF16)


def _kernel(x_ref, g_ref, wq_ref, wk_ref, wv_ref, wo_ref, tab_ref, y_ref,
            xb, a_s, wkv_s, wq_s, wo_s, gs, cs, q_s, kvb, kvo, top_s, mix_s, at_own, at_par, acc, yst,
            ld, kv_sem, wq_sem, wo_sem, xs_sem, xr_sem, kvs_sem, kvr_sem, fs_sem, as_sem, ar_sem, ys_sem, yr_sem):
    me = lax.axis_index("sp")
    z, c = lax.div(me, 2), lax.rem(me, 2)
    partner = 2 * z + 1 - c
    d = a_s.shape[1]
    half = d // 2
    own = pl.multiple_of(c * T, T)
    oth = pl.multiple_of((1 - c) * T, T)
    col0 = pl.multiple_of(c * half, half)
    col1 = pl.multiple_of((1 - c) * half, half)
    slabs = half // W

    def copy(src, dst, sem):
        return pltpu.make_async_copy(src, dst, sem)

    def remote(src, dst, ssem, rsem, to):
        return pltpu.make_async_remote_copy(src_ref=src, dst_ref=dst, send_sem=ssem, recv_sem=rsem, device_id={"sp": to}, device_id_type=MESH)

    load_x = copy(x_ref, xb.at[pl.ds(own, T)], ld.at[0])
    load_t = copy(tab_ref.at[:, pl.ds(pl.multiple_of(z * C, C), C)], cs, ld.at[1])
    load_g = copy(g_ref, gs, ld.at[2])

    def load_kv(n):
        rows = pl.ds(n * half, half)
        return [copy(w.at[rows], wkv_s.at[rows, pl.ds(i * 2 * HEAD, 2 * HEAD)], kv_sem.at[n, i]) for i, w in enumerate((wk_ref, wv_ref))]

    def load_q(i):
        return copy(wq_ref.at[:, pl.ds(pl.multiple_of(col0 + i * W, W), W)], wq_s.at[i], wq_sem.at[i])

    def load_o(p, i):
        return copy(wo_ref.at[pl.ds(col1 if p else col0, half), pl.ds(pl.multiple_of(col0 + i * W, W), W)], wo_s.at[p, i], wo_sem.at[p, i])

    load_x.start()
    load_g.start()

    barrier = pltpu.get_barrier_semaphore()
    pl.semaphore_signal(barrier, inc=1, device_id={"sp": partner}, device_id_type=MESH)

    @pl.when(z > 0)
    def _():
        for o in range(2):
            pl.semaphore_signal(barrier, inc=1, device_id={"sp": 2 * z - 2 + o}, device_id_type=MESH)

    for one in (*load_kv(0), *load_kv(1), load_t):
        one.start()
    send_x = remote(xb.at[pl.ds(own, T)], xb.at[pl.ds(own, T)], xs_sem, xr_sem, partner)
    load_x.wait()
    load_g.wait()

    def send():
        @pl.when(z < Z - 1)
        def _():
            pl.semaphore_wait(barrier, 3)

        @pl.when(z == Z - 1)
        def _():
            pl.semaphore_wait(barrier, 1)

        send_x.start()

    @pl.when(z > 0)
    def _():
        send()

    def norm(start):
        gain = gs[...].astype(F32).reshape(1, d)

        def rows(i, _):
            for r in range(2):
                here = pl.ds(pl.multiple_of(start + (2 * i + r) * 16, 16), 16)
                wide = xb[here, :].astype(F32)
                scale = lax.rsqrt(jnp.mean(wide * wide, -1, keepdims=True) + 1e-6)
                a_s[here, :] = (wide * scale * gain).astype(BF16)

        lax.fori_loop(0, T // 32, rows, None)

    norm(own)

    @pl.when(z == 0)
    def _():
        send()

    load_q(0).start()
    mine = a_s[pl.ds(own, T), :]
    for one in load_kv(0):
        one.wait()
    acc[:T, :W] = _dot(mine[:, :half], wkv_s[:half])
    for one in load_kv(1):
        one.wait()
    load_t.wait()
    load_q(1).start()
    kv = (acc[:T, :W] + _dot(mine[:, half:], wkv_s[half:])).astype(BF16)
    k, v = kv[:, : 2 * HEAD].astype(F32), kv[:, 2 * HEAD :]
    cos, sin = cs[0, pl.ds(own, T), :], cs[1, pl.ds(own, T), :]
    k0, k1 = _turn(k[:, :HEAD], cos, sin), _turn(k[:, HEAD:], cos, sin)
    v0, v1 = v[:, :HEAD], v[:, HEAD:]
    rows_of = lambda t: pl.ds(pl.multiple_of(t * T, T), T)

    @pl.when(c == 0)
    def _():
        kvb[0, rows_of(me), :], kvb[1, rows_of(me), :], kvo[0], kvo[1] = k0, v0, k1, v1

    @pl.when(c == 1)
    def _():
        kvb[0, rows_of(me), :], kvb[1, rows_of(me), :], kvo[0], kvo[1] = k1, v1, k0, v0

    def piece(t):
        return kvb.at[:, rows_of(t)]

    to_pair = remote(kvo, piece(me), kvs_sem.at[0], kvr_sem.at[me], partner)
    to_next = remote(piece(me), piece(me), kvs_sem.at[1], kvr_sem.at[me], 2 * z + 2 + c)
    to_cross = remote(kvo, piece(me), kvs_sem.at[2], kvr_sem.at[me], 2 * z + 3 - c)

    @pl.when(z < Z - 1)
    def _():
        to_next.start()
        to_cross.start()

    to_pair.start()

    def arrived(t):
        remote(piece(t), piece(t), kvs_sem.at[0], kvr_sem.at[t], partner).wait_recv()

    def forward(t):
        return remote(piece(t), piece(t), fs_sem.at[t], kvr_sem.at[t], 2 * z + 2 + c)

    def pass_on(back, which):
        t = 2 * (z - back) + (c if which == 0 else 1 - c)

        @pl.when((z >= back) & (z < Z - 1))
        def _():
            arrived(t)
            forward(t).start()

    def raw(i, start, n):
        return _dot(a_s[pl.ds(start, n), :], wq_s[i])

    def queries(q, i, start, n):
        here = pl.ds(start, n)
        q = q.astype(BF16).astype(F32)
        cos, sin = cs[0, here, :], cs[1, here, :]
        for h in range(W // HEAD):
            q_s[i * (W // HEAD) + h, here, :] = _turn(q[:, h * HEAD : (h + 1) * HEAD], cos, sin)

    load_q(2).start()
    send_x.wait_recv()
    norm(oth)
    load_q(0).wait()
    load_q(3).start()
    middle = (z > 0) & (z < Z - 1)

    @pl.when(middle)
    def _():
        for i, (back, which) in enumerate(((1, 0), (1, 1), (2, 0), (2, 1))):
            if i:
                load_q(i).wait()
            if i == slabs - 1:
                load_o(0, 0).start()
                load_o(0, 1).start()
            queries(raw(i, 0, C), i, 0, C)
            pass_on(back, which)

    @pl.when(jnp.logical_not(middle))
    def _():
        q0 = raw(0, 0, C)
        load_q(1).wait()
        q1 = raw(1, 0, C)
        queries(q0, 0, 0, C)
        load_q(2).wait()
        q2 = raw(2, 0, C)
        queries(q1, 1, 0, C)
        load_q(3).wait()
        load_o(0, 0).start()
        load_o(0, 1).start()
        q3 = raw(3, 0, C)
        queries(q2, 2, 0, C)
        queries(q3, 3, 0, C)

    for i in range(2, slabs):
        load_o(0, i).start()

    e = HEAD**-0.5 * LOG2E
    strip = 2 * C
    strips = QH * C // strip

    def send_at(n):
        there = pl.ds(n * W, W)
        return remote(at_own.at[:, there], at_par.at[:, there], as_sem.at[n], ar_sem.at[n], partner)

    def finish_heads(s, mix):
        out = (mix[:HEAD] * (1 / mix[HEAD : HEAD + 1])).astype(BF16).T
        for h in range(2):
            at_own[:, (2 * s + h) * HEAD : (2 * s + h + 1) * HEAD] = out[h * C : (h + 1) * C]
        if s % 2:
            send_at(s // 2).start()

    def block(j, n, ahead, first, last):
        size = n * C
        here = pl.ds(pl.multiple_of(j * C, C), size)
        keys = kvb[0, here, :]
        values = jnp.concatenate([kvb[1, here, :].T, jnp.ones((8, size), BF16)], axis=0)
        waiting = []

        def scores(s):
            if s < strips:
                waiting.append(_dot(keys, q_s[2 * s : 2 * s + 2].reshape(strip, HEAD), 1, 1))

        if first:
            seen = lax.broadcasted_iota(jnp.int32, (T, T), 1) >= lax.broadcasted_iota(jnp.int32, (T, T), 0)
            none = jnp.zeros((T, T), BF16)

        def own_weights(sc):
            weights, tops = [], []
            for q in range(strip // T):
                keep = size - (T if q % 2 == 0 else 0)
                part = sc[:keep, q * T : (q + 1) * T]
                edge = jnp.where(seen, part[keep - T :], HIDDEN)
                part = edge if keep == T else jnp.concatenate([part[: keep - T], edge], axis=0)
                top = part.max(axis=0, keepdims=True)
                p = jnp.exp2((part - top) * e).astype(BF16)
                weights.append(p if keep == size else jnp.concatenate([p, none], axis=0))
                tops.append(top)
            return jnp.concatenate(weights, axis=1), jnp.concatenate(tops, axis=1)

        for s in range(ahead):
            scores(s)
        for s in range(strips):
            scores(s + ahead)
            sc = waiting.pop(0)
            at = slice(s * strip, (s + 1) * strip)
            if first:
                p, top = own_weights(sc)
                mix = _dot(values, p)
            else:
                old = top_s[:, at]
                top = jnp.maximum(old, sc.max(axis=0, keepdims=True))
                mix = mix_s[:, at] * jnp.exp2((old - top) * e) + _dot(values, jnp.exp2((sc - top) * e).astype(BF16))
            if last:
                if s:
                    finish_heads(s - 1, done)
                done = mix
            else:
                mix_s[:, at] = mix
                top_s[:, at] = top

        if last:
            finish_heads(strips - 1, done)

    arrived(partner)

    @pl.when(z == 0)
    def _():
        block(z, 1, 3, True, False)

    @pl.when(z > 0)
    def _():
        @pl.when(z == Z - 1)
        def _():
            arrived(2 * z - 2)
            arrived(2 * z - 1)

        block(z - 1, 2, 3, True, False)

    for i in range(slabs):
        load_o(1, i).start()

    @pl.when(z == Z - 1)
    def _():
        arrived(2)
        arrived(3)
        block(1, 1, 3, False, False)
        arrived(0)
        arrived(1)

    @pl.when(z > 1)
    def _():
        block(0, 1, 3, False, True)

    @pl.when(z < 2)
    def _():
        for s in range(strips):
            finish_heads(s, mix_s[:, s * strip : (s + 1) * strip])

    for p in range(2):
        for i in range(slabs):
            load_o(p, i).wait()
    for i in range(slabs):
        acc[:, i * W : (i + 1) * W] = _dot(at_own[...], wo_s[0, i])
    for n in range(slabs):
        send_at(n).wait_recv()

    def cols(core, i):
        return pl.ds(pl.multiple_of(core * half + i * W, W), W)

    def send_y(i):
        return remote(yst.at[i, pl.ds(oth, T)], y_ref.at[:, cols(c, i)], ys_sem.at[i], yr_sem.at[i], partner)

    def take_y(i):
        return remote(yst.at[i, pl.ds(oth, T)], y_ref.at[:, cols(1 - c, i)], ys_sem.at[i], yr_sem.at[i], partner)

    def finish(i, start, n, y):
        here = pl.ds(start, n)
        yst[i, here, :] = (xb[here, cols(c, i)].astype(F32) + (acc[here, i * W : (i + 1) * W] + y)).astype(BF16)

    last = slabs - 1
    parts = [(i, 0, C) for i in range(last)] + [(last, oth, T), (last, own, T)]
    y = _dot(at_par[...], wo_s[1, 0])
    for n, (i, start, size) in enumerate(parts):
        if n + 1 < len(parts):
            j, at, m = parts[n + 1]
            ahead = _dot(at_par[pl.ds(at, m), :], wo_s[1, j])
        finish(i, start, size, y)
        y = ahead
        if n != len(parts) - 1:
            send_y(i).start()
        if i < last or start is own:
            y_ref[:, cols(c, i)] = yst[i, pl.ds(own, T), :]

    send_x.wait_send()
    to_pair.wait_send()

    @pl.when(z < Z - 1)
    def _():
        to_next.wait_send()
        to_cross.wait_send()
        lax.fori_loop(0, 2 * z, lambda t, _: forward(t).wait_send(), None)

    for n in range(slabs):
        send_at(n).wait_send()
        send_y(n).wait_send()
        take_y(n).wait_recv()


def _table(rows):
    half = HEAD // 2
    angle = np.arange(rows, dtype=np.float64)[:, None] * float(THETA) ** (-np.arange(half, dtype=np.float64) / half)
    cos, sin = np.cos(angle), np.sin(angle)
    return np.stack([np.concatenate([cos, cos], 1), np.concatenate([-sin, sin], 1)]).astype(np.float32)


def solution(mesh):
    def step(x, gain, wq, wk, wv, wo):
        d = x.shape[1]
        half = d // 2
        slabs = half // W
        hbm = pl.BlockSpec(memory_space=pl.ANY)
        vm = pltpu.VMEM
        dma = pltpu.SemaphoreType.DMA
        scratch = [
            vm((C, d), BF16), vm((C, d), BF16), vm((d, 4 * HEAD), BF16),
            vm((slabs, d, W), BF16), vm((2, slabs, half, W), BF16), vm((d,), BF16), vm((2, C, HEAD), F32), vm((QH, C, HEAD), BF16),
            vm((2, Z * C, HEAD), BF16), vm((2, T, HEAD), BF16), vm((1, QH * C), F32), vm((HEAD + 8, QH * C), F32),
            vm((C, half), BF16), vm((C, half), BF16), vm((C, half), F32), vm((slabs, C, W), BF16),
            dma((3,)), dma((2, 2)), dma((slabs,)), dma((2, slabs)), dma, dma, dma((3,)), dma((2 * Z,)), dma((2 * Z,)),
            dma((slabs,)), dma((slabs,)), dma((slabs,)), dma((slabs,)),
        ]
        return pl.pallas_call(
            _kernel,
            out_shape=pltpu.VMEM(x.shape, x.dtype),
            in_specs=[hbm] * 7,
            out_specs=pl.BlockSpec(memory_space=pltpu.VMEM),
            scratch_shapes=scratch,
            compiler_params=pltpu.CompilerParams(collective_id=0, has_side_effects=True, vmem_limit_bytes=60 * 2**20),
            name="layer",
        )(x, gain, wq, wk, wv, wo, jnp.asarray(_table(Z * C)))

    tokens, whole = P(("dp", "sp"), None), P(None, None)
    return jax.shard_map(
        step,
        mesh=mesh,
        in_specs=(tokens, P(None), whole, whole, whole, whole),
        out_specs=tokens,
        check_vma=False,
    )
```

```python
import functools
import math

import jax
import jax.numpy as jnp
import numpy as np
from jax import lax
from jax.experimental import pallas as pl
from jax.experimental.pallas import tpu as pltpu
from jax.sharding import PartitionSpec as P

HEAD = 128
THETA = 10000
HIDDEN = -2e30
LOG2E = 1.4426950408889634
MESH = pl.DeviceIdType.MESH
F32, BF16 = jnp.float32, jnp.bfloat16
T = 128
C = 2 * T
W = 512
Z = 4
QH = 16


def _dot(a, b, ca=1, cb=0):
    return lax.dot_general(a, b, (((ca,), (cb,)), ((), ())), preferred_element_type=F32)


def _turn(t, cos, sin):
    return (t * cos + pltpu.roll(t, HEAD // 2, 1) * sin).astype(BF16)


def _kernel(x_ref, g_ref, wq_ref, wk_ref, wv_ref, wo_ref, tab_ref, y_ref,
            xb, a_s, wkv_s, wq_s, wo_s, gs, cs, q_s, kvb, kvo, top_s, mix_s, at_own, at_par, acc, yst,
            ld, kv_sem, wq_sem, wo_sem, xs_sem, xr_sem, kvs_sem, kvr_sem, fs_sem, as_sem, ar_sem, ys_sem, yr_sem):
    me = lax.axis_index("sp")
    z, c = lax.div(me, 2), lax.rem(me, 2)
    partner = 2 * z + 1 - c
    d = a_s.shape[1]
    half = d // 2
    own = pl.multiple_of(c * T, T)
    oth = pl.multiple_of((1 - c) * T, T)
    col0 = pl.multiple_of(c * half, half)
    col1 = pl.multiple_of((1 - c) * half, half)
    slabs = half // W

    def copy(src, dst, sem):
        return pltpu.make_async_copy(src, dst, sem)

    def remote(src, dst, ssem, rsem, to):
        return pltpu.make_async_remote_copy(src_ref=src, dst_ref=dst, send_sem=ssem, recv_sem=rsem, device_id={"sp": to}, device_id_type=MESH)

    load_x = copy(x_ref, xb.at[pl.ds(own, T)], ld.at[0])
    load_t = copy(tab_ref.at[:, pl.ds(pl.multiple_of(z * C, C), C)], cs, ld.at[1])
    load_g = copy(g_ref, gs, ld.at[2])

    def load_kv(n):
        rows = pl.ds(n * half, half)
        return [copy(w.at[rows], wkv_s.at[rows, pl.ds(i * 2 * HEAD, 2 * HEAD)], kv_sem.at[n, i]) for i, w in enumerate((wk_ref, wv_ref))]

    def load_q(i):
        return copy(wq_ref.at[:, pl.ds(pl.multiple_of(col0 + i * W, W), W)], wq_s.at[i], wq_sem.at[i])

    def load_o(p, i):
        return copy(wo_ref.at[pl.ds(col1 if p else col0, half), pl.ds(pl.multiple_of(col0 + i * W, W), W)], wo_s.at[p, i], wo_sem.at[p, i])

    load_x.start()
    load_g.start()

    barrier = pltpu.get_barrier_semaphore()
    pl.semaphore_signal(barrier, inc=1, device_id={"sp": partner}, device_id_type=MESH)

    @pl.when(z > 0)
    def _():
        for o in range(2):
            pl.semaphore_signal(barrier, inc=1, device_id={"sp": 2 * z - 2 + o}, device_id_type=MESH)

    for one in (*load_kv(0), *load_kv(1), load_t):
        one.start()
    load_q(0).start(priority=1)
    send_x = remote(xb.at[pl.ds(own, T)], xb.at[pl.ds(own, T)], xs_sem, xr_sem, partner)
    load_x.wait()
    load_g.wait()

    def send():
        @pl.when(z < Z - 1)
        def _():
            pl.semaphore_wait(barrier, 3)

        @pl.when(z == Z - 1)
        def _():
            pl.semaphore_wait(barrier, 1)

        send_x.start()

    @pl.when(z > 0)
    def _():
        send()

    def norm(start):
        gain = gs[...].astype(F32).reshape(1, d)

        def rows(i, _):
            for r in range(2):
                here = pl.ds(pl.multiple_of(start + (2 * i + r) * 16, 16), 16)
                wide = xb[here, :].astype(F32)
                scale = lax.rsqrt(jnp.mean(wide * wide, -1, keepdims=True) + 1e-6)
                a_s[here, :] = (wide * scale * gain).astype(BF16)

        lax.fori_loop(0, T // 32, rows, None)

    norm(own)

    @pl.when(z == 0)
    def _():
        send()

    mine = a_s[pl.ds(own, T), :]
    for one in load_kv(0):
        one.wait()
    acc[:T, :W] = _dot(mine[:, :half], wkv_s[:half])
    for one in load_kv(1):
        one.wait()
    load_t.wait()
    load_q(1).start(priority=1)
    kv = (acc[:T, :W] + _dot(mine[:, half:], wkv_s[half:])).astype(BF16)
    k, v = kv[:, : 2 * HEAD].astype(F32), kv[:, 2 * HEAD :]
    cos, sin = cs[0, pl.ds(own, T), :], cs[1, pl.ds(own, T), :]
    k0, k1 = _turn(k[:, :HEAD], cos, sin), _turn(k[:, HEAD:], cos, sin)
    v0, v1 = v[:, :HEAD], v[:, HEAD:]
    rows_of = lambda t: pl.ds(pl.multiple_of(t * T, T), T)

    @pl.when(c == 0)
    def _():
        kvb[0, rows_of(me), :], kvb[1, rows_of(me), :], kvo[0], kvo[1] = k0, v0, k1, v1

    @pl.when(c == 1)
    def _():
        kvb[0, rows_of(me), :], kvb[1, rows_of(me), :], kvo[0], kvo[1] = k1, v1, k0, v0

    def piece(t):
        return kvb.at[:, rows_of(t)]

    to_pair = remote(kvo, piece(me), kvs_sem.at[0], kvr_sem.at[me], partner)
    to_next = remote(piece(me), piece(me), kvs_sem.at[1], kvr_sem.at[me], 2 * z + 2 + c)
    to_cross = remote(kvo, piece(me), kvs_sem.at[2], kvr_sem.at[me], 2 * z + 3 - c)

    @pl.when(z < Z - 1)
    def _():
        to_next.start()
        to_cross.start()

    to_pair.start()

    def arrived(t):
        remote(piece(t), piece(t), kvs_sem.at[0], kvr_sem.at[t], partner).wait_recv()

    def forward(t):
        return remote(piece(t), piece(t), fs_sem.at[t], kvr_sem.at[t], 2 * z + 2 + c)

    def pass_on(chip, back, which):
        t = 2 * (z - back) + (c if which == 0 else 1 - c)

        @pl.when(z == chip)
        def _():
            arrived(t)
            forward(t).start()

    def raw(i, start, n):
        return _dot(a_s[pl.ds(start, n), :], wq_s[i])

    def queries(q, i, start, n):
        here = pl.ds(start, n)
        q = q.astype(BF16).astype(F32)
        cos, sin = cs[0, here, :], cs[1, here, :]
        for h in range(W // HEAD):
            q_s[i * (W // HEAD) + h, here, :] = _turn(q[:, h * HEAD : (h + 1) * HEAD], cos, sin)

    send_x.wait_recv()
    norm(oth)
    load_q(2).start(priority=1)
    load_q(0).wait()
    middle = (z > 0) & (z < Z - 1)

    @pl.when(middle)
    def _():
        for i, passing in enumerate((((1, 1, 0),), ((1, 1, 1), (2, 1, 0)), ((2, 1, 1), (2, 2, 0)), ((2, 2, 1),))):
            if i:
                load_q(i).wait()
            if i == slabs - 1:
                load_o(0, 0).start(priority=1)
                load_o(0, 1).start(priority=1)
            queries(raw(i, 0, C), i, 0, C)
            if i == 0:
                load_q(3).start(priority=1)
            for at in passing:
                pass_on(*at)

    @pl.when(jnp.logical_not(middle))
    def _():
        q0 = raw(0, 0, C)
        load_q(3).start(priority=1)
        load_q(1).wait()
        q1 = raw(1, 0, C)
        queries(q0, 0, 0, C)
        load_q(2).wait()
        q2 = raw(2, 0, C)
        queries(q1, 1, 0, C)
        load_q(3).wait()
        load_o(0, 0).start(priority=1)
        load_o(0, 1).start(priority=1)
        q3 = raw(3, 0, C)
        queries(q2, 2, 0, C)
        queries(q3, 3, 0, C)

    for i in range(2, slabs):
        load_o(0, i).start(priority=1)

    e = HEAD**-0.5 * LOG2E
    strip = 2 * C
    strips = QH * C // strip

    def send_at(n):
        there = pl.ds(n * W, W)
        return remote(at_own.at[:, there], at_par.at[:, there], as_sem.at[n], ar_sem.at[n], partner)

    def finish_heads(s, mix):
        out = (mix[:HEAD] * (1 / mix[HEAD : HEAD + 1])).astype(BF16).T
        for h in range(2):
            at_own[:, (2 * s + h) * HEAD : (2 * s + h + 1) * HEAD] = out[h * C : (h + 1) * C]
        if s % 2:
            send_at(s // 2).start()

    def block(j, n, ahead, first, last):
        size = n * C
        here = pl.ds(pl.multiple_of(j * C, C), size)
        keys = kvb[0, here, :]
        values = jnp.concatenate([kvb[1, here, :].T, jnp.ones((8, size), BF16)], axis=0)
        waiting = []

        def scores(s):
            if s < strips:
                waiting.append(_dot(keys, q_s[2 * s : 2 * s + 2].reshape(strip, HEAD), 1, 1))

        if first:
            seen = lax.broadcasted_iota(jnp.int32, (T, T), 1) >= lax.broadcasted_iota(jnp.int32, (T, T), 0)
            none = jnp.zeros((T, T), BF16)

        def own_weights(sc):
            weights, tops = [], []
            for q in range(strip // T):
                keep = size - (T if q % 2 == 0 else 0)
                part = sc[:keep, q * T : (q + 1) * T]
                edge = jnp.where(seen, part[keep - T :], HIDDEN)
                part = edge if keep == T else jnp.concatenate([part[: keep - T], edge], axis=0)
                top = part.max(axis=0, keepdims=True)
                p = jnp.exp2((part - top) * e).astype(BF16)
                weights.append(p if keep == size else jnp.concatenate([p, none], axis=0))
                tops.append(top)
            return jnp.concatenate(weights, axis=1), jnp.concatenate(tops, axis=1)

        for s in range(ahead):
            scores(s)
        for s in range(strips):
            scores(s + ahead)
            sc = waiting.pop(0)
            at = slice(s * strip, (s + 1) * strip)
            if first:
                p, top = own_weights(sc)
                mix = _dot(values, p)
            else:
                old = top_s[:, at]
                top = jnp.maximum(old, sc.max(axis=0, keepdims=True))
                mix = mix_s[:, at] * jnp.exp2((old - top) * e) + _dot(values, jnp.exp2((sc - top) * e).astype(BF16))
            if last:
                if s:
                    finish_heads(s - 1, done)
                done = mix
            else:
                mix_s[:, at] = mix
                top_s[:, at] = top

        if last:
            finish_heads(strips - 1, done)

    arrived(partner)

    @pl.when(z == 0)
    def _():
        block(z, 1, 3, True, False)

    @pl.when(z > 0)
    def _():
        @pl.when(z == Z - 1)
        def _():
            arrived(2 * z - 2)
            arrived(2 * z - 1)

        block(z - 1, 2, 3, True, False)

    for i in range(slabs):
        load_o(1, i).start(priority=1)

    @pl.when(z == Z - 1)
    def _():
        arrived(2)
        arrived(3)
        block(1, 1, 3, False, False)
        arrived(0)
        arrived(1)

    @pl.when(z > 1)
    def _():
        block(0, 1, 3, False, True)

    @pl.when(z < 2)
    def _():
        for s in range(strips):
            finish_heads(s, mix_s[:, s * strip : (s + 1) * strip])

    for i in range(slabs):
        load_o(0, i).wait()
    for i in range(slabs):
        acc[:, i * W : (i + 1) * W] = _dot(at_own[...], wo_s[0, i])
    for n in range(slabs):
        send_at(n).wait_recv()
        load_o(1, n).wait()

    def cols(core, i):
        return pl.ds(pl.multiple_of(core * half + i * W, W), W)

    def send_y(i):
        return remote(yst.at[i, pl.ds(oth, T)], y_ref.at[:, cols(c, i)], ys_sem.at[i], yr_sem.at[i], partner)

    def take_y(i):
        return remote(yst.at[i, pl.ds(oth, T)], y_ref.at[:, cols(1 - c, i)], ys_sem.at[i], yr_sem.at[i], partner)

    def finish(i, start, n, y):
        here = pl.ds(start, n)
        yst[i, here, :] = (xb[here, cols(c, i)].astype(F32) + (acc[here, i * W : (i + 1) * W] + y)).astype(BF16)

    last = slabs - 1
    parts = [(i, 0, C) for i in range(last)] + [(last, oth, T), (last, own, T)]
    y = _dot(at_par[...], wo_s[1, 0])
    for n, (i, start, size) in enumerate(parts):
        if n + 1 < len(parts):
            j, at, m = parts[n + 1]
            ahead = _dot(at_par[pl.ds(at, m), :], wo_s[1, j])
        finish(i, start, size, y)
        y = ahead
        if n != len(parts) - 1:
            send_y(i).start()
        if i < last or start is own:
            y_ref[:, cols(c, i)] = yst[i, pl.ds(own, T), :]

    send_x.wait_send()
    to_pair.wait_send()

    @pl.when(z < Z - 1)
    def _():
        to_next.wait_send()
        to_cross.wait_send()
        lax.fori_loop(0, 2 * z, lambda t, _: forward(t).wait_send(), None)

    for n in range(slabs):
        send_at(n).wait_send()
        send_y(n).wait_send()
        take_y(n).wait_recv()


def _table(rows):
    half = HEAD // 2
    angle = np.arange(rows, dtype=np.float64)[:, None] * float(THETA) ** (-np.arange(half, dtype=np.float64) / half)
    cos, sin = np.cos(angle), np.sin(angle)
    return np.stack([np.concatenate([cos, cos], 1), np.concatenate([-sin, sin], 1)]).astype(np.float32)


def solution(mesh):
    def step(x, gain, wq, wk, wv, wo):
        d = x.shape[1]
        half = d // 2
        slabs = half // W
        hbm = pl.BlockSpec(memory_space=pl.ANY)
        vm = pltpu.VMEM
        dma = pltpu.SemaphoreType.DMA
        scratch = [
            vm((C, d), BF16), vm((C, d), BF16), vm((d, 4 * HEAD), BF16),
            vm((slabs, d, W), BF16), vm((2, slabs, half, W), BF16), vm((d,), BF16), vm((2, C, HEAD), F32), vm((QH, C, HEAD), BF16),
            vm((2, Z * C, HEAD), BF16), vm((2, T, HEAD), BF16), vm((1, QH * C), F32), vm((HEAD + 8, QH * C), F32),
            vm((C, half), BF16), vm((C, half), BF16), vm((C, half), F32), vm((slabs, C, W), BF16),
            dma((3,)), dma((2, 2)), dma((slabs,)), dma((2, slabs)), dma, dma, dma((3,)), dma((2 * Z,)), dma((2 * Z,)),
            dma((slabs,)), dma((slabs,)), dma((slabs,)), dma((slabs,)),
        ]
        return pl.pallas_call(
            _kernel,
            out_shape=pltpu.VMEM(x.shape, x.dtype),
            in_specs=[hbm] * 7,
            out_specs=pl.BlockSpec(memory_space=pltpu.VMEM),
            scratch_shapes=scratch,
            compiler_params=pltpu.CompilerParams(collective_id=0, has_side_effects=True, vmem_limit_bytes=60 * 2**20),
            name="layer",
        )(x, gain, wq, wk, wv, wo, jnp.asarray(_table(Z * C)))

    tokens, whole = P(("dp", "sp"), None), P(None, None)
    return jax.shard_map(
        step,
        mesh=mesh,
        in_specs=(tokens, P(None), whole, whole, whole, whole),
        out_specs=tokens,
        check_vma=False,
    )
```

```python
import functools
import math

import jax
import jax.numpy as jnp
import numpy as np
from jax import lax
from jax.experimental import pallas as pl
from jax.experimental.pallas import tpu as pltpu
from jax.sharding import PartitionSpec as P

HEAD = 128
THETA = 10000
HIDDEN = -2e30
LOG2E = 1.4426950408889634
MESH = pl.DeviceIdType.MESH
F32, BF16 = jnp.float32, jnp.bfloat16
T = 128
C = 2 * T
W = 512
Z = 4
QH = 16


def _dot(a, b, ca=1, cb=0):
    return lax.dot_general(a, b, (((ca,), (cb,)), ((), ())), preferred_element_type=F32)


def _turn(t, cos, sin):
    return (t * cos + pltpu.roll(t, HEAD // 2, 1) * sin).astype(BF16)


def _kernel(x_ref, g_ref, wq_ref, wk_ref, wv_ref, wo_ref, tab_ref, y_ref,
            xb, a_s, wkv_s, wq_s, wo_s, gs, cs, q_s, kvb, kvo, top_s, mix_s, at_own, at_par, acc, yst,
            ld, kv_sem, wq_sem, wo_sem, xs_sem, xr_sem, kvs_sem, kvr_sem, fs_sem, as_sem, ar_sem, ys_sem, yr_sem):
    me = lax.axis_index("sp")
    z, c = lax.div(me, 2), lax.rem(me, 2)
    partner = 2 * z + 1 - c
    d = a_s.shape[1]
    half = d // 2
    own = pl.multiple_of(c * T, T)
    oth = pl.multiple_of((1 - c) * T, T)
    col0 = pl.multiple_of(c * half, half)
    col1 = pl.multiple_of((1 - c) * half, half)
    slabs = half // W

    def copy(src, dst, sem):
        return pltpu.make_async_copy(src, dst, sem)

    def remote(src, dst, ssem, rsem, to):
        return pltpu.make_async_remote_copy(src_ref=src, dst_ref=dst, send_sem=ssem, recv_sem=rsem, device_id={"sp": to}, device_id_type=MESH)

    load_x = copy(x_ref, xb.at[pl.ds(own, T)], ld.at[0])
    load_t = copy(tab_ref.at[:, pl.ds(pl.multiple_of(z * C, C), C)], cs, ld.at[1])
    load_g = copy(g_ref, gs, ld.at[2])

    def load_kv(n):
        rows = pl.ds(n * half, half)
        return [copy(w.at[rows], wkv_s.at[rows, pl.ds(i * 2 * HEAD, 2 * HEAD)], kv_sem.at[n, i]) for i, w in enumerate((wk_ref, wv_ref))]

    def load_q(i):
        return copy(wq_ref.at[:, pl.ds(pl.multiple_of(col0 + i * W, W), W)], wq_s.at[i], wq_sem.at[i])

    def load_o(p, i):
        return copy(wo_ref.at[pl.ds(col1 if p else col0, half), pl.ds(pl.multiple_of(col0 + i * W, W), W)], wo_s.at[p, i], wo_sem.at[p, i])

    load_x.start()
    load_g.start()

    barrier = pltpu.get_barrier_semaphore()
    pl.semaphore_signal(barrier, inc=1, device_id={"sp": partner}, device_id_type=MESH)

    @pl.when(z > 0)
    def _():
        for o in range(2):
            pl.semaphore_signal(barrier, inc=1, device_id={"sp": 2 * z - 2 + o}, device_id_type=MESH)

    for one in (*load_kv(0), *load_kv(1), load_t):
        one.start()
    load_q(0).start(priority=1)
    send_x = remote(xb.at[pl.ds(own, T)], xb.at[pl.ds(own, T)], xs_sem, xr_sem, partner)
    load_x.wait()
    load_g.wait()

    def send():
        @pl.when(z < Z - 1)
        def _():
            pl.semaphore_wait(barrier, 3)

        @pl.when(z == Z - 1)
        def _():
            pl.semaphore_wait(barrier, 1)

        send_x.start()

    @pl.when(z > 0)
    def _():
        send()

    def norm(start):
        gain = gs[...].astype(F32).reshape(1, d)

        def rows(i, _):
            for r in range(2):
                here = pl.ds(pl.multiple_of(start + (2 * i + r) * 16, 16), 16)
                wide = xb[here, :].astype(F32)
                scale = lax.rsqrt(jnp.mean(wide * wide, -1, keepdims=True) + 1e-6)
                a_s[here, :] = (wide * scale * gain).astype(BF16)

        lax.fori_loop(0, T // 32, rows, None)

    norm(own)

    @pl.when(z == 0)
    def _():
        send()

    mine = a_s[pl.ds(own, T), :]
    for one in load_kv(0):
        one.wait()
    acc[:T, :W] = _dot(mine[:, :half], wkv_s[:half])
    for one in load_kv(1):
        one.wait()
    load_t.wait()
    load_q(1).start(priority=1)
    kv = (acc[:T, :W] + _dot(mine[:, half:], wkv_s[half:])).astype(BF16)
    k, v = kv[:, : 2 * HEAD].astype(F32), kv[:, 2 * HEAD :]
    cos, sin = cs[0, pl.ds(own, T), :], cs[1, pl.ds(own, T), :]
    k0, k1 = _turn(k[:, :HEAD], cos, sin), _turn(k[:, HEAD:], cos, sin)
    v0, v1 = v[:, :HEAD], v[:, HEAD:]
    rows_of = lambda t: pl.ds(pl.multiple_of(t * T, T), T)

    @pl.when(c == 0)
    def _():
        kvb[0, rows_of(me), :], kvb[1, rows_of(me), :], kvo[0], kvo[1] = k0, v0, k1, v1

    @pl.when(c == 1)
    def _():
        kvb[0, rows_of(me), :], kvb[1, rows_of(me), :], kvo[0], kvo[1] = k1, v1, k0, v0

    def piece(t):
        return kvb.at[:, rows_of(t)]

    to_pair = remote(kvo, piece(me), kvs_sem.at[0], kvr_sem.at[me], partner)
    to_next = remote(piece(me), piece(me), kvs_sem.at[1], kvr_sem.at[me], 2 * z + 2 + c)
    to_cross = remote(kvo, piece(me), kvs_sem.at[2], kvr_sem.at[me], 2 * z + 3 - c)

    @pl.when(z < Z - 1)
    def _():
        to_next.start()
        to_cross.start()

    to_pair.start()

    def arrived(t):
        remote(piece(t), piece(t), kvs_sem.at[0], kvr_sem.at[t], partner).wait_recv()

    def forward(t):
        return remote(piece(t), piece(t), fs_sem.at[t], kvr_sem.at[t], 2 * z + 2 + c)

    def pass_on(back, which):
        t = 2 * (z - back) + (c if which == 0 else 1 - c)

        @pl.when((z >= back) & (z < Z - 1))
        def _():
            arrived(t)
            forward(t).start()

    def raw(i, start, n):
        return _dot(a_s[pl.ds(start, n), :], wq_s[i])

    def queries(q, i, start, n):
        here = pl.ds(start, n)
        q = q.astype(BF16).astype(F32)
        cos, sin = cs[0, here, :], cs[1, here, :]
        for h in range(W // HEAD):
            q_s[i * (W // HEAD) + h, here, :] = _turn(q[:, h * HEAD : (h + 1) * HEAD], cos, sin)

    send_x.wait_recv()
    norm(oth)
    load_q(2).start(priority=1)
    load_q(0).wait()
    middle = (z > 0) & (z < Z - 1)

    @pl.when(middle)
    def _():
        for i, (back, which) in enumerate(((1, 0), (1, 1), (2, 0), (2, 1))):
            if i:
                load_q(i).wait()
            if i == slabs - 1:
                load_o(0, 0).start(priority=1)
                load_o(0, 1).start(priority=1)
            queries(raw(i, 0, C), i, 0, C)
            if i == 0:
                load_q(3).start(priority=1)
            pass_on(back, which)

    @pl.when(jnp.logical_not(middle))
    def _():
        q0 = raw(0, 0, C)
        load_q(3).start(priority=1)
        load_q(1).wait()
        q1 = raw(1, 0, C)
        queries(q0, 0, 0, C)
        load_q(2).wait()
        q2 = raw(2, 0, C)
        queries(q1, 1, 0, C)
        load_q(3).wait()
        load_o(0, 0).start(priority=1)
        load_o(0, 1).start(priority=1)
        q3 = raw(3, 0, C)
        queries(q2, 2, 0, C)
        queries(q3, 3, 0, C)

    for i in range(2, slabs):
        load_o(0, i).start(priority=1)

    e = HEAD**-0.5 * LOG2E
    strip = 2 * C
    strips = QH * C // strip

    def send_at(n):
        there = pl.ds(n * W, W)
        return remote(at_own.at[:, there], at_par.at[:, there], as_sem.at[n], ar_sem.at[n], partner)

    def finish_heads(s, mix):
        out = (mix[:HEAD] * (1 / mix[HEAD : HEAD + 1])).astype(BF16).T
        for h in range(2):
            at_own[:, (2 * s + h) * HEAD : (2 * s + h + 1) * HEAD] = out[h * C : (h + 1) * C]
        if s % 2:
            send_at(s // 2).start()

    def block(j, n, ahead, first, last):
        size = n * C
        here = pl.ds(pl.multiple_of(j * C, C), size)
        keys = kvb[0, here, :]
        values = jnp.concatenate([kvb[1, here, :].T, jnp.ones((8, size), BF16)], axis=0)
        waiting = []

        def scores(s):
            if s < strips:
                waiting.append(_dot(keys, q_s[2 * s : 2 * s + 2].reshape(strip, HEAD), 1, 1))

        if first:
            seen = lax.broadcasted_iota(jnp.int32, (T, T), 1) >= lax.broadcasted_iota(jnp.int32, (T, T), 0)
            none = jnp.zeros((T, T), BF16)

        def own_weights(sc):
            weights, tops = [], []
            for q in range(strip // T):
                keep = size - (T if q % 2 == 0 else 0)
                part = sc[:keep, q * T : (q + 1) * T]
                edge = jnp.where(seen, part[keep - T :], HIDDEN)
                part = edge if keep == T else jnp.concatenate([part[: keep - T], edge], axis=0)
                top = part.max(axis=0, keepdims=True)
                p = jnp.exp2((part - top) * e).astype(BF16)
                weights.append(p if keep == size else jnp.concatenate([p, none], axis=0))
                tops.append(top)
            return jnp.concatenate(weights, axis=1), jnp.concatenate(tops, axis=1)

        for s in range(ahead):
            scores(s)
        for s in range(strips):
            scores(s + ahead)
            sc = waiting.pop(0)
            at = slice(s * strip, (s + 1) * strip)
            if first:
                p, top = own_weights(sc)
                mix = _dot(values, p)
            else:
                old = top_s[:, at]
                top = jnp.maximum(old, sc.max(axis=0, keepdims=True))
                mix = mix_s[:, at] * jnp.exp2((old - top) * e) + _dot(values, jnp.exp2((sc - top) * e).astype(BF16))
            if last:
                if s:
                    finish_heads(s - 1, done)
                done = mix
            else:
                mix_s[:, at] = mix
                top_s[:, at] = top

        if last:
            finish_heads(strips - 1, done)

    arrived(partner)

    @pl.when(z == 0)
    def _():
        block(z, 1, 3, True, False)

    @pl.when(z > 0)
    def _():
        @pl.when(z == Z - 1)
        def _():
            arrived(2 * z - 2)
            arrived(2 * z - 1)

        block(z - 1, 2, 3, True, False)

    for i in range(slabs):
        load_o(1, i).start(priority=1)

    @pl.when(z == Z - 1)
    def _():
        arrived(2)
        arrived(3)
        block(1, 1, 3, False, False)
        arrived(0)
        arrived(1)

    @pl.when(z > 1)
    def _():
        block(0, 1, 3, False, True)

    @pl.when(z < 2)
    def _():
        for s in range(strips):
            finish_heads(s, mix_s[:, s * strip : (s + 1) * strip])

    for i in range(slabs):
        load_o(0, i).wait()
    for i in range(slabs):
        acc[:, i * W : (i + 1) * W] = _dot(at_own[...], wo_s[0, i])
    for n in range(slabs):
        send_at(n).wait_recv()
        load_o(1, n).wait()

    def cols(core, i):
        return pl.ds(pl.multiple_of(core * half + i * W, W), W)

    def send_y(i):
        return remote(yst.at[i, pl.ds(oth, T)], y_ref.at[:, cols(c, i)], ys_sem.at[i], yr_sem.at[i], partner)

    def take_y(i):
        return remote(yst.at[i, pl.ds(oth, T)], y_ref.at[:, cols(1 - c, i)], ys_sem.at[i], yr_sem.at[i], partner)

    def finish(i, start, n, y):
        here = pl.ds(start, n)
        yst[i, here, :] = (xb[here, cols(c, i)].astype(F32) + (acc[here, i * W : (i + 1) * W] + y)).astype(BF16)

    def run(parts):
        y = None
        for n, (i, start, size) in enumerate(parts):
            if n == 0:
                y = _dot(at_par[pl.ds(start, size), :], wo_s[1, i])
            if n + 1 < len(parts):
                j, at, m = parts[n + 1]
                ahead = _dot(at_par[pl.ds(at, m), :], wo_s[1, j])
            finish(i, start, size, y)
            y = ahead
            if start is not own:
                send_y(i).start()
            if start is not oth:
                y_ref[:, cols(c, i)] = yst[i, pl.ds(own, T), :]

    late = range(slabs // 2, slabs)
    run([(i, 0, C) for i in range(slabs // 2)] + [(i, oth, T) for i in late])

    @pl.when(z >= 0)
    def _():
        run([(i, own, T) for i in late])

    send_x.wait_send()
    to_pair.wait_send()

    @pl.when(z < Z - 1)
    def _():
        to_next.wait_send()
        to_cross.wait_send()
        lax.fori_loop(0, 2 * z, lambda t, _: forward(t).wait_send(), None)

    for n in range(slabs):
        send_at(n).wait_send()
        send_y(n).wait_send()
        take_y(n).wait_recv()


def _table(rows):
    half = HEAD // 2
    angle = np.arange(rows, dtype=np.float64)[:, None] * float(THETA) ** (-np.arange(half, dtype=np.float64) / half)
    cos, sin = np.cos(angle), np.sin(angle)
    return np.stack([np.concatenate([cos, cos], 1), np.concatenate([-sin, sin], 1)]).astype(np.float32)


def solution(mesh):
    def step(x, gain, wq, wk, wv, wo):
        d = x.shape[1]
        half = d // 2
        slabs = half // W
        hbm = pl.BlockSpec(memory_space=pl.ANY)
        vm = pltpu.VMEM
        dma = pltpu.SemaphoreType.DMA
        scratch = [
            vm((C, d), BF16), vm((C, d), BF16), vm((d, 4 * HEAD), BF16),
            vm((slabs, d, W), BF16), vm((2, slabs, half, W), BF16), vm((d,), BF16), vm((2, C, HEAD), F32), vm((QH, C, HEAD), BF16),
            vm((2, Z * C, HEAD), BF16), vm((2, T, HEAD), BF16), vm((1, QH * C), F32), vm((HEAD + 8, QH * C), F32),
            vm((C, half), BF16), vm((C, half), BF16), vm((C, half), F32), vm((slabs, C, W), BF16),
            dma((3,)), dma((2, 2)), dma((slabs,)), dma((2, slabs)), dma, dma, dma((3,)), dma((2 * Z,)), dma((2 * Z,)),
            dma((slabs,)), dma((slabs,)), dma((slabs,)), dma((slabs,)),
        ]
        return pl.pallas_call(
            _kernel,
            out_shape=pltpu.VMEM(x.shape, x.dtype),
            in_specs=[hbm] * 7,
            out_specs=pl.BlockSpec(memory_space=pltpu.VMEM),
            scratch_shapes=scratch,
            compiler_params=pltpu.CompilerParams(collective_id=0, has_side_effects=True, vmem_limit_bytes=60 * 2**20),
            name="layer",
        )(x, gain, wq, wk, wv, wo, jnp.asarray(_table(Z * C)))

    tokens, whole = P(("dp", "sp"), None), P(None, None)
    return jax.shard_map(
        step,
        mesh=mesh,
        in_specs=(tokens, P(None), whole, whole, whole, whole),
        out_specs=tokens,
        check_vma=False,
    )
```

```python
import functools
import math

import jax
import jax.numpy as jnp
import numpy as np
from jax import lax
from jax.experimental import pallas as pl
from jax.experimental.pallas import tpu as pltpu
from jax.sharding import PartitionSpec as P

HEAD = 128
THETA = 10000
HIDDEN = -2e30
LOG2E = 1.4426950408889634
MESH = pl.DeviceIdType.MESH
F32, BF16 = jnp.float32, jnp.bfloat16
T = 128
C = 2 * T
W = 512
Z = 4
QH = 16


def _dot(a, b, ca=1, cb=0):
    return lax.dot_general(a, b, (((ca,), (cb,)), ((), ())), preferred_element_type=F32)


def _turn(t, cos, sin):
    return (t * cos + pltpu.roll(t, HEAD // 2, 1) * sin).astype(BF16)


def _kernel(x_ref, g_ref, wq_ref, wk_ref, wv_ref, wo_ref, tab_ref, y_ref,
            xb, a_s, wkv_s, wq_s, wo_s, gs, cs, q_s, kvb, kvo, top_s, mix_s, at_own, at_par, acc, yst,
            ld, kv_sem, wq_sem, wo_sem, xs_sem, xr_sem, kvs_sem, kvr_sem, fs_sem, as_sem, ar_sem, ys_sem, yr_sem):
    me = lax.axis_index("sp")
    z, c = lax.div(me, 2), lax.rem(me, 2)
    partner = 2 * z + 1 - c
    d = a_s.shape[1]
    half = d // 2
    own = pl.multiple_of(c * T, T)
    oth = pl.multiple_of((1 - c) * T, T)
    col0 = pl.multiple_of(c * half, half)
    col1 = pl.multiple_of((1 - c) * half, half)
    slabs = half // W

    def copy(src, dst, sem):
        return pltpu.make_async_copy(src, dst, sem)

    def remote(src, dst, ssem, rsem, to):
        return pltpu.make_async_remote_copy(src_ref=src, dst_ref=dst, send_sem=ssem, recv_sem=rsem, device_id={"sp": to}, device_id_type=MESH)

    load_x = copy(x_ref, xb.at[pl.ds(own, T)], ld.at[0])
    load_t = copy(tab_ref.at[:, pl.ds(pl.multiple_of(z * C, C), C)], cs, ld.at[1])
    load_g = copy(g_ref, gs, ld.at[2])

    def load_kv(n):
        rows = pl.ds(n * half, half)
        return [copy(w.at[rows], wkv_s.at[rows, pl.ds(i * 2 * HEAD, 2 * HEAD)], kv_sem.at[n, i]) for i, w in enumerate((wk_ref, wv_ref))]

    def load_q(i):
        return copy(wq_ref.at[:, pl.ds(pl.multiple_of(col0 + i * W, W), W)], wq_s.at[i], wq_sem.at[i])

    def load_o(p, i):
        return copy(wo_ref.at[pl.ds(col1 if p else col0, half), pl.ds(pl.multiple_of(col0 + i * W, W), W)], wo_s.at[p, i], wo_sem.at[p, i])

    load_x.start()
    load_g.start()

    barrier = pltpu.get_barrier_semaphore()
    pl.semaphore_signal(barrier, inc=1, device_id={"sp": partner}, device_id_type=MESH)

    @pl.when(z > 0)
    def _():
        for o in range(2):
            pl.semaphore_signal(barrier, inc=1, device_id={"sp": 2 * z - 2 + o}, device_id_type=MESH)

    for one in (*load_kv(0), *load_kv(1), load_t):
        one.start()
    load_q(0).start(priority=1)
    send_x = remote(xb.at[pl.ds(own, T)], xb.at[pl.ds(own, T)], xs_sem, xr_sem, partner)
    load_x.wait()
    load_g.wait()

    def send():
        @pl.when(z < Z - 1)
        def _():
            pl.semaphore_wait(barrier, 3)

        @pl.when(z == Z - 1)
        def _():
            pl.semaphore_wait(barrier, 1)

        send_x.start()

    @pl.when(z > 0)
    def _():
        send()

    def norm(start):
        gain = gs[...].astype(F32).reshape(1, d)

        def rows(i, _):
            for r in range(2):
                here = pl.ds(pl.multiple_of(start + (2 * i + r) * 16, 16), 16)
                wide = xb[here, :].astype(F32)
                scale = lax.rsqrt(jnp.mean(wide * wide, -1, keepdims=True) + 1e-6)
                a_s[here, :] = (wide * scale * gain).astype(BF16)

        lax.fori_loop(0, T // 32, rows, None)

    norm(own)

    @pl.when(z == 0)
    def _():
        send()

    mine = a_s[pl.ds(own, T), :]
    for one in load_kv(0):
        one.wait()
    acc[:T, :W] = _dot(mine[:, :half], wkv_s[:half])
    for one in load_kv(1):
        one.wait()
    load_t.wait()
    load_q(1).start(priority=1)
    kv = (acc[:T, :W] + _dot(mine[:, half:], wkv_s[half:])).astype(BF16)
    k, v = kv[:, : 2 * HEAD].astype(F32), kv[:, 2 * HEAD :]
    cos, sin = cs[0, pl.ds(own, T), :], cs[1, pl.ds(own, T), :]
    k0, k1 = _turn(k[:, :HEAD], cos, sin), _turn(k[:, HEAD:], cos, sin)
    v0, v1 = v[:, :HEAD], v[:, HEAD:]
    rows_of = lambda t: pl.ds(pl.multiple_of(t * T, T), T)

    @pl.when(c == 0)
    def _():
        kvb[0, rows_of(me), :], kvb[1, rows_of(me), :], kvo[0], kvo[1] = k0, v0, k1, v1

    @pl.when(c == 1)
    def _():
        kvb[0, rows_of(me), :], kvb[1, rows_of(me), :], kvo[0], kvo[1] = k1, v1, k0, v0

    def piece(t):
        return kvb.at[:, rows_of(t)]

    to_pair = remote(kvo, piece(me), kvs_sem.at[0], kvr_sem.at[me], partner)
    to_next = remote(piece(me), piece(me), kvs_sem.at[1], kvr_sem.at[me], 2 * z + 2 + c)
    to_cross = remote(kvo, piece(me), kvs_sem.at[2], kvr_sem.at[me], 2 * z + 3 - c)

    @pl.when(z < Z - 1)
    def _():
        to_next.start()
        to_cross.start()

    to_pair.start()

    def arrived(t):
        remote(piece(t), piece(t), kvs_sem.at[0], kvr_sem.at[t], partner).wait_recv()

    def forward(t):
        return remote(piece(t), piece(t), fs_sem.at[t], kvr_sem.at[t], 2 * z + 2 + c)

    def pass_on(back, which):
        t = 2 * (z - back) + (c if which == 0 else 1 - c)

        @pl.when((z >= back) & (z < Z - 1))
        def _():
            arrived(t)
            forward(t).start()

    def raw(i, start, n):
        return _dot(a_s[pl.ds(start, n), :], wq_s[i])

    def queries(q, i, start, n):
        here = pl.ds(start, n)
        q = q.astype(BF16).astype(F32)
        cos, sin = cs[0, here, :], cs[1, here, :]
        for h in range(W // HEAD):
            q_s[i * (W // HEAD) + h, here, :] = _turn(q[:, h * HEAD : (h + 1) * HEAD], cos, sin)

    send_x.wait_recv()
    norm(oth)
    load_q(2).start(priority=1)
    load_q(0).wait()
    middle = (z > 0) & (z < Z - 1)

    @pl.when(middle)
    def _():
        for i, (back, which) in enumerate(((1, 0), (1, 1), (2, 0), (2, 1))):
            if i:
                load_q(i).wait()
            if i == slabs - 1:
                load_o(0, 0).start(priority=1)
                load_o(0, 1).start(priority=1)
            queries(raw(i, 0, C), i, 0, C)
            if i == 0:
                load_q(3).start(priority=1)
            pass_on(back, which)

    @pl.when(jnp.logical_not(middle))
    def _():
        q0 = raw(0, 0, C)
        load_q(3).start(priority=1)
        load_q(1).wait()
        q1 = raw(1, 0, C)
        queries(q0, 0, 0, C)
        load_q(2).wait()
        q2 = raw(2, 0, C)
        queries(q1, 1, 0, C)
        load_q(3).wait()
        load_o(0, 0).start(priority=1)
        load_o(0, 1).start(priority=1)
        q3 = raw(3, 0, C)
        queries(q2, 2, 0, C)
        queries(q3, 3, 0, C)

    for i in range(2, slabs):
        load_o(0, i).start(priority=1)

    e = HEAD**-0.5 * LOG2E
    strip = 2 * C
    strips = QH * C // strip

    def send_at(n):
        there = pl.ds(n * W, W)
        return remote(at_own.at[:, there], at_par.at[:, there], as_sem.at[n], ar_sem.at[n], partner)

    def finish_heads(s, mix):
        out = (mix[:HEAD] * (1 / mix[HEAD : HEAD + 1])).astype(BF16).T
        for h in range(2):
            at_own[:, (2 * s + h) * HEAD : (2 * s + h + 1) * HEAD] = out[h * C : (h + 1) * C]
        if s % 2:
            send_at(s // 2).start()

    def project(i, second):
        there, rows = slice(i * W, (i + 1) * W), slice(half // 2, half) if second else slice(0, half // 2)
        y = _dot(at_own[:, rows], wo_s[0, i, rows, :])
        acc[:, there] = acc[:, there] + y if second else y

    def block(j, n, ahead, first, last):
        size = n * C
        here = pl.ds(pl.multiple_of(j * C, C), size)
        keys = kvb[0, here, :]
        values = jnp.concatenate([kvb[1, here, :].T, jnp.ones((8, size), BF16)], axis=0)
        waiting = []

        def scores(s):
            if s < strips:
                waiting.append(_dot(keys, q_s[2 * s : 2 * s + 2].reshape(strip, HEAD), 1, 1))

        if first:
            seen = lax.broadcasted_iota(jnp.int32, (T, T), 1) >= lax.broadcasted_iota(jnp.int32, (T, T), 0)
            none = jnp.zeros((T, T), BF16)

        def own_weights(sc):
            weights, tops = [], []
            for q in range(strip // T):
                keep = size - (T if q % 2 == 0 else 0)
                part = sc[:keep, q * T : (q + 1) * T]
                edge = jnp.where(seen, part[keep - T :], HIDDEN)
                part = edge if keep == T else jnp.concatenate([part[: keep - T], edge], axis=0)
                top = part.max(axis=0, keepdims=True)
                p = jnp.exp2((part - top) * e).astype(BF16)
                weights.append(p if keep == size else jnp.concatenate([p, none], axis=0))
                tops.append(top)
            return jnp.concatenate(weights, axis=1), jnp.concatenate(tops, axis=1)

        for s in range(ahead):
            scores(s)
        for s in range(strips):
            scores(s + ahead)
            sc = waiting.pop(0)
            at = slice(s * strip, (s + 1) * strip)
            if first:
                p, top = own_weights(sc)
                mix = _dot(values, p)
            else:
                old = top_s[:, at]
                top = jnp.maximum(old, sc.max(axis=0, keepdims=True))
                mix = mix_s[:, at] * jnp.exp2((old - top) * e) + _dot(values, jnp.exp2((sc - top) * e).astype(BF16))
            if last:
                if s:
                    finish_heads(s - 1, done)
                if s >= strips // 2:
                    project(s - strips // 2, False)
                done = mix
            else:
                mix_s[:, at] = mix
                top_s[:, at] = top

        if last:
            finish_heads(strips - 1, done)

    arrived(partner)

    @pl.when(z == 0)
    def _():
        block(z, 1, 3, True, False)

    @pl.when(z > 0)
    def _():
        @pl.when(z == Z - 1)
        def _():
            arrived(2 * z - 2)
            arrived(2 * z - 1)

        block(z - 1, 2, 3, True, False)

    for i in range(slabs):
        load_o(1, i).start(priority=1)

    @pl.when(z == Z - 1)
    def _():
        arrived(2)
        arrived(3)
        block(1, 1, 3, False, False)
        arrived(0)
        arrived(1)

    for i in range(slabs):
        load_o(0, i).wait()

    @pl.when(z > 1)
    def _():
        block(0, 1, 3, False, True)

    @pl.when(z < 2)
    def _():
        for s in range(strips):
            finish_heads(s, mix_s[:, s * strip : (s + 1) * strip])
        for i in range(slabs):
            project(i, False)

    for i in range(slabs):
        project(i, True)
    for n in range(slabs):
        send_at(n).wait_recv()
        load_o(1, n).wait()

    def cols(core, i):
        return pl.ds(pl.multiple_of(core * half + i * W, W), W)

    def send_y(i):
        return remote(yst.at[i, pl.ds(oth, T)], y_ref.at[:, cols(c, i)], ys_sem.at[i], yr_sem.at[i], partner)

    def take_y(i):
        return remote(yst.at[i, pl.ds(oth, T)], y_ref.at[:, cols(1 - c, i)], ys_sem.at[i], yr_sem.at[i], partner)

    def finish(i, start, n, y):
        here = pl.ds(start, n)
        yst[i, here, :] = (xb[here, cols(c, i)].astype(F32) + (acc[here, i * W : (i + 1) * W] + y)).astype(BF16)

    def run(parts):
        y = None
        for n, (i, start, size) in enumerate(parts):
            if n == 0:
                y = _dot(at_par[pl.ds(start, size), :], wo_s[1, i])
            if n + 1 < len(parts):
                j, at, m = parts[n + 1]
                ahead = _dot(at_par[pl.ds(at, m), :], wo_s[1, j])
            finish(i, start, size, y)
            y = ahead
            if start is not own:
                send_y(i).start()
            if start is not oth:
                y_ref[:, cols(c, i)] = yst[i, pl.ds(own, T), :]

    late = range(slabs // 2, slabs)
    run([(i, 0, C) for i in range(slabs // 2)] + [(i, oth, T) for i in late])

    @pl.when(z >= 0)
    def _():
        run([(i, own, T) for i in late])

    send_x.wait_send()
    to_pair.wait_send()

    @pl.when(z < Z - 1)
    def _():
        to_next.wait_send()
        to_cross.wait_send()
        lax.fori_loop(0, 2 * z, lambda t, _: forward(t).wait_send(), None)

    for n in range(slabs):
        send_at(n).wait_send()
        send_y(n).wait_send()
        take_y(n).wait_recv()


def _table(rows):
    half = HEAD // 2
    angle = np.arange(rows, dtype=np.float64)[:, None] * float(THETA) ** (-np.arange(half, dtype=np.float64) / half)
    cos, sin = np.cos(angle), np.sin(angle)
    return np.stack([np.concatenate([cos, cos], 1), np.concatenate([-sin, sin], 1)]).astype(np.float32)


def solution(mesh):
    def step(x, gain, wq, wk, wv, wo):
        d = x.shape[1]
        half = d // 2
        slabs = half // W
        hbm = pl.BlockSpec(memory_space=pl.ANY)
        vm = pltpu.VMEM
        dma = pltpu.SemaphoreType.DMA
        scratch = [
            vm((C, d), BF16), vm((C, d), BF16), vm((d, 4 * HEAD), BF16),
            vm((slabs, d, W), BF16), vm((2, slabs, half, W), BF16), vm((d,), BF16), vm((2, C, HEAD), F32), vm((QH, C, HEAD), BF16),
            vm((2, Z * C, HEAD), BF16), vm((2, T, HEAD), BF16), vm((1, QH * C), F32), vm((HEAD + 8, QH * C), F32),
            vm((C, half), BF16), vm((C, half), BF16), vm((C, half), F32), vm((slabs, C, W), BF16),
            dma((3,)), dma((2, 2)), dma((slabs,)), dma((2, slabs)), dma, dma, dma((3,)), dma((2 * Z,)), dma((2 * Z,)),
            dma((slabs,)), dma((slabs,)), dma((slabs,)), dma((slabs,)),
        ]
        return pl.pallas_call(
            _kernel,
            out_shape=pltpu.VMEM(x.shape, x.dtype),
            in_specs=[hbm] * 7,
            out_specs=pl.BlockSpec(memory_space=pltpu.VMEM),
            scratch_shapes=scratch,
            compiler_params=pltpu.CompilerParams(collective_id=0, has_side_effects=True, vmem_limit_bytes=60 * 2**20),
            name="layer",
        )(x, gain, wq, wk, wv, wo, jnp.asarray(_table(Z * C)))

    tokens, whole = P(("dp", "sp"), None), P(None, None)
    return jax.shard_map(
        step,
        mesh=mesh,
        in_specs=(tokens, P(None), whole, whole, whole, whole),
        out_specs=tokens,
        check_vma=False,
    )
```

```python
import functools
import math

import jax
import jax.numpy as jnp
import numpy as np
from jax import lax
from jax.experimental import pallas as pl
from jax.experimental.pallas import tpu as pltpu
from jax.sharding import PartitionSpec as P

HEAD = 128
THETA = 10000
HIDDEN = -2e30
LOG2E = 1.4426950408889634
MESH = pl.DeviceIdType.MESH
F32, BF16 = jnp.float32, jnp.bfloat16
T = 128
C = 2 * T
W = 512
Z = 4
QH = 16


def _dot(a, b, ca=1, cb=0):
    return lax.dot_general(a, b, (((ca,), (cb,)), ((), ())), preferred_element_type=F32)


def _turn(t, cos, sin):
    return (t * cos + pltpu.roll(t, HEAD // 2, 1) * sin).astype(BF16)


def _kernel(x_ref, g_ref, wq_ref, wk_ref, wv_ref, wo_ref, tab_ref, y_ref,
            xb, a_s, wkv_s, wq_s, wo_s, gs, cs, q_s, kvb, kvo, top_s, mix_s, at_own, at_par, acc, yst,
            ld, kv_sem, wq_sem, wo_sem, xs_sem, xr_sem, kvs_sem, kvr_sem, fs_sem, as_sem, ar_sem, ys_sem, yr_sem):
    me = lax.axis_index("sp")
    z, c = lax.div(me, 2), lax.rem(me, 2)
    partner = 2 * z + 1 - c
    d = a_s.shape[1]
    half = d // 2
    own = pl.multiple_of(c * T, T)
    oth = pl.multiple_of((1 - c) * T, T)
    col0 = pl.multiple_of(c * half, half)
    col1 = pl.multiple_of((1 - c) * half, half)
    slabs = half // W

    def copy(src, dst, sem):
        return pltpu.make_async_copy(src, dst, sem)

    def remote(src, dst, ssem, rsem, to):
        return pltpu.make_async_remote_copy(src_ref=src, dst_ref=dst, send_sem=ssem, recv_sem=rsem, device_id={"sp": to}, device_id_type=MESH)

    load_x = copy(x_ref, xb.at[pl.ds(own, T)], ld.at[0])
    load_t = copy(tab_ref.at[:, pl.ds(pl.multiple_of(z * C, C), C)], cs, ld.at[1])
    load_g = copy(g_ref, gs, ld.at[2])

    def load_kv(n):
        rows = pl.ds(n * half, half)
        return [copy(w.at[rows], wkv_s.at[rows, pl.ds(i * 2 * HEAD, 2 * HEAD)], kv_sem.at[n, i]) for i, w in enumerate((wk_ref, wv_ref))]

    def load_q(i):
        return copy(wq_ref.at[:, pl.ds(pl.multiple_of(col0 + i * W, W), W)], wq_s.at[i], wq_sem.at[i])

    def load_o(p, i):
        return copy(wo_ref.at[pl.ds(col1 if p else col0, half), pl.ds(pl.multiple_of(col0 + i * W, W), W)], wo_s.at[p, i], wo_sem.at[p, i])

    load_x.start()
    load_g.start()

    barrier = pltpu.get_barrier_semaphore()
    pl.semaphore_signal(barrier, inc=1, device_id={"sp": partner}, device_id_type=MESH)

    @pl.when(z > 0)
    def _():
        for o in range(2):
            pl.semaphore_signal(barrier, inc=1, device_id={"sp": 2 * z - 2 + o}, device_id_type=MESH)

    for one in (*load_kv(0), *load_kv(1), load_t):
        one.start()
    load_q(0).start(priority=1)
    send_x = remote(xb.at[pl.ds(own, T)], xb.at[pl.ds(own, T)], xs_sem, xr_sem, partner)
    load_x.wait()
    load_g.wait()

    def send_when(here, signals):
        @pl.when(here)
        def _():
            pl.semaphore_wait(barrier, signals)
            send_x.start()

    def norm(start, first=0, last=T // 32):
        gain = gs[...].astype(F32).reshape(1, d)

        def rows(i, _):
            for r in range(2):
                here = pl.ds(pl.multiple_of(start + (2 * i + r) * 16, 16), 16)
                wide = xb[here, :].astype(F32)
                scale = lax.rsqrt(jnp.mean(wide * wide, -1, keepdims=True) + 1e-6)
                a_s[here, :] = (wide * scale * gain).astype(BF16)

        lax.fori_loop(first, last, rows, None)

    send_when(z == Z - 1, 1)
    norm(own, 0, T // 64)
    send_when((z > 0) & (z < Z - 1), 3)
    norm(own, T // 64, T // 32)
    send_when(z == 0, 3)

    mine = a_s[pl.ds(own, T), :]
    for one in load_kv(0):
        one.wait()
    acc[:T, :W] = _dot(mine[:, :half], wkv_s[:half])
    for one in load_kv(1):
        one.wait()
    load_t.wait()
    load_q(1).start(priority=1)
    kv = (acc[:T, :W] + _dot(mine[:, half:], wkv_s[half:])).astype(BF16)
    k, v = kv[:, : 2 * HEAD].astype(F32), kv[:, 2 * HEAD :]
    cos, sin = cs[0, pl.ds(own, T), :], cs[1, pl.ds(own, T), :]
    k0, k1 = _turn(k[:, :HEAD], cos, sin), _turn(k[:, HEAD:], cos, sin)
    v0, v1 = v[:, :HEAD], v[:, HEAD:]
    rows_of = lambda t: pl.ds(pl.multiple_of(t * T, T), T)

    @pl.when(c == 0)
    def _():
        kvb[0, rows_of(me), :], kvb[1, rows_of(me), :], kvo[0], kvo[1] = k0, v0, k1, v1

    @pl.when(c == 1)
    def _():
        kvb[0, rows_of(me), :], kvb[1, rows_of(me), :], kvo[0], kvo[1] = k1, v1, k0, v0

    def piece(t):
        return kvb.at[:, rows_of(t)]

    to_pair = remote(kvo, piece(me), kvs_sem.at[0], kvr_sem.at[me], partner)
    to_next = remote(piece(me), piece(me), kvs_sem.at[1], kvr_sem.at[me], 2 * z + 2 + c)
    to_cross = remote(kvo, piece(me), kvs_sem.at[2], kvr_sem.at[me], 2 * z + 3 - c)

    @pl.when(z < Z - 1)
    def _():
        to_next.start()
        to_cross.start()

    to_pair.start()

    def arrived(t):
        remote(piece(t), piece(t), kvs_sem.at[0], kvr_sem.at[t], partner).wait_recv()

    def forward(t):
        return remote(piece(t), piece(t), fs_sem.at[t], kvr_sem.at[t], 2 * z + 2 + c)

    def pass_on(back, which):
        t = 2 * (z - back) + (c if which == 0 else 1 - c)

        @pl.when((z >= back) & (z < Z - 1))
        def _():
            arrived(t)
            forward(t).start()

    def raw(i, start, n):
        return _dot(a_s[pl.ds(start, n), :], wq_s[i])

    def queries(q, i, start, n):
        here = pl.ds(start, n)
        q = q.astype(BF16).astype(F32)
        cos, sin = cs[0, here, :], cs[1, here, :]
        for h in range(W // HEAD):
            q_s[i * (W // HEAD) + h, here, :] = _turn(q[:, h * HEAD : (h + 1) * HEAD], cos, sin)

    send_x.wait_recv()
    norm(oth)
    load_q(2).start(priority=1)
    load_q(0).wait()
    middle = (z > 0) & (z < Z - 1)

    @pl.when(middle)
    def _():
        for i, (back, which) in enumerate(((1, 0), (1, 1), (2, 0), (2, 1))):
            if i:
                load_q(i).wait()
            if i == slabs - 1:
                load_o(0, 0).start(priority=1)
                load_o(0, 1).start(priority=1)
            queries(raw(i, 0, C), i, 0, C)
            if i == 0:
                load_q(3).start(priority=1)
            pass_on(back, which)

    @pl.when(jnp.logical_not(middle))
    def _():
        q0 = raw(0, 0, C)
        load_q(3).start(priority=1)
        load_q(1).wait()
        q1 = raw(1, 0, C)
        queries(q0, 0, 0, C)
        load_q(2).wait()
        q2 = raw(2, 0, C)
        queries(q1, 1, 0, C)
        load_q(3).wait()
        load_o(0, 0).start(priority=1)
        load_o(0, 1).start(priority=1)
        q3 = raw(3, 0, C)
        queries(q2, 2, 0, C)
        queries(q3, 3, 0, C)

    for i in range(2, slabs):
        load_o(0, i).start(priority=1)

    e = HEAD**-0.5 * LOG2E
    strip = 2 * C
    strips = QH * C // strip

    def send_at(n):
        there = pl.ds(n * W, W)
        return remote(at_own.at[:, there], at_par.at[:, there], as_sem.at[n], ar_sem.at[n], partner)

    def finish_heads(s, mix):
        out = (mix[:HEAD] * (1 / mix[HEAD : HEAD + 1])).astype(BF16).T
        for h in range(2):
            at_own[:, (2 * s + h) * HEAD : (2 * s + h + 1) * HEAD] = out[h * C : (h + 1) * C]
        if s % 2:
            send_at(s // 2).start()

    def block(j, n, ahead, first, last):
        size = n * C
        here = pl.ds(pl.multiple_of(j * C, C), size)
        keys = kvb[0, here, :]
        values = jnp.concatenate([kvb[1, here, :].T, jnp.ones((8, size), BF16)], axis=0)
        waiting = []

        def scores(s):
            if s < strips:
                waiting.append(_dot(keys, q_s[2 * s : 2 * s + 2].reshape(strip, HEAD), 1, 1))

        if first:
            seen = lax.broadcasted_iota(jnp.int32, (T, T), 1) >= lax.broadcasted_iota(jnp.int32, (T, T), 0)
            none = jnp.zeros((T, T), BF16)

        def own_weights(sc):
            weights, tops = [], []
            for q in range(strip // T):
                keep = size - (T if q % 2 == 0 else 0)
                part = sc[:keep, q * T : (q + 1) * T]
                edge = jnp.where(seen, part[keep - T :], HIDDEN)
                part = edge if keep == T else jnp.concatenate([part[: keep - T], edge], axis=0)
                top = part.max(axis=0, keepdims=True)
                p = jnp.exp2((part - top) * e).astype(BF16)
                weights.append(p if keep == size else jnp.concatenate([p, none], axis=0))
                tops.append(top)
            return jnp.concatenate(weights, axis=1), jnp.concatenate(tops, axis=1)

        for s in range(ahead):
            scores(s)
        for s in range(strips):
            scores(s + ahead)
            sc = waiting.pop(0)
            at = slice(s * strip, (s + 1) * strip)
            if first:
                p, top = own_weights(sc)
                mix = _dot(values, p)
            else:
                old = top_s[:, at]
                top = jnp.maximum(old, sc.max(axis=0, keepdims=True))
                mix = mix_s[:, at] * jnp.exp2((old - top) * e) + _dot(values, jnp.exp2((sc - top) * e).astype(BF16))
            if last:
                if s:
                    finish_heads(s - 1, done)
                done = mix
            else:
                mix_s[:, at] = mix
                top_s[:, at] = top

        if last:
            finish_heads(strips - 1, done)

    arrived(partner)

    @pl.when(z == 0)
    def _():
        block(z, 1, 3, True, False)

    @pl.when(z > 0)
    def _():
        @pl.when(z == Z - 1)
        def _():
            arrived(2 * z - 2)
            arrived(2 * z - 1)

        block(z - 1, 2, 3, True, False)

    for i in range(slabs):
        load_o(1, i).start(priority=1)

    @pl.when(z == Z - 1)
    def _():
        arrived(2)
        arrived(3)
        block(1, 1, 3, False, False)
        arrived(0)
        arrived(1)

    @pl.when(z > 1)
    def _():
        block(0, 1, 2, False, True)

    @pl.when(z < 2)
    def _():
        for s in range(strips):
            finish_heads(s, mix_s[:, s * strip : (s + 1) * strip])

    for i in range(slabs):
        load_o(0, i).wait()
    for i in range(slabs):
        acc[:, i * W : (i + 1) * W] = _dot(at_own[...], wo_s[0, i])
    for n in range(slabs):
        send_at(n).wait_recv()
        load_o(1, n).wait()

    def cols(core, i):
        return pl.ds(pl.multiple_of(core * half + i * W, W), W)

    def send_y(i):
        return remote(yst.at[i, pl.ds(oth, T)], y_ref.at[:, cols(c, i)], ys_sem.at[i], yr_sem.at[i], partner)

    def take_y(i):
        return remote(yst.at[i, pl.ds(oth, T)], y_ref.at[:, cols(1 - c, i)], ys_sem.at[i], yr_sem.at[i], partner)

    def finish(i, start, n, y):
        here = pl.ds(start, n)
        yst[i, here, :] = (xb[here, cols(c, i)].astype(F32) + (acc[here, i * W : (i + 1) * W] + y)).astype(BF16)

    def run(parts):
        y = None
        for n, (i, start, size) in enumerate(parts):
            if n == 0:
                y = _dot(at_par[pl.ds(start, size), :], wo_s[1, i])
            if n + 1 < len(parts):
                j, at, m = parts[n + 1]
                ahead = _dot(at_par[pl.ds(at, m), :], wo_s[1, j])
            finish(i, start, size, y)
            y = ahead
            if start is not own:
                send_y(i).start()
            if start is not oth:
                y_ref[:, cols(c, i)] = yst[i, pl.ds(own, T), :]

    late = range(slabs // 2, slabs)
    run([(i, 0, C) for i in range(slabs // 2)] + [(i, oth, T) for i in late])

    @pl.when(z >= 0)
    def _():
        run([(i, own, T) for i in late])

    send_x.wait_send()
    to_pair.wait_send()

    @pl.when(z < Z - 1)
    def _():
        to_next.wait_send()
        to_cross.wait_send()
        lax.fori_loop(0, 2 * z, lambda t, _: forward(t).wait_send(), None)

    for n in range(slabs):
        send_at(n).wait_send()
        send_y(n).wait_send()
        take_y(n).wait_recv()


def _table(rows):
    half = HEAD // 2
    angle = np.arange(rows, dtype=np.float64)[:, None] * float(THETA) ** (-np.arange(half, dtype=np.float64) / half)
    cos, sin = np.cos(angle), np.sin(angle)
    return np.stack([np.concatenate([cos, cos], 1), np.concatenate([-sin, sin], 1)]).astype(np.float32)


def solution(mesh):
    def step(x, gain, wq, wk, wv, wo):
        d = x.shape[1]
        half = d // 2
        slabs = half // W
        hbm = pl.BlockSpec(memory_space=pl.ANY)
        vm = pltpu.VMEM
        dma = pltpu.SemaphoreType.DMA
        scratch = [
            vm((C, d), BF16), vm((C, d), BF16), vm((d, 4 * HEAD), BF16),
            vm((slabs, d, W), BF16), vm((2, slabs, half, W), BF16), vm((d,), BF16), vm((2, C, HEAD), F32), vm((QH, C, HEAD), BF16),
            vm((2, Z * C, HEAD), BF16), vm((2, T, HEAD), BF16), vm((1, QH * C), F32), vm((HEAD + 8, QH * C), F32),
            vm((C, half), BF16), vm((C, half), BF16), vm((C, half), F32), vm((slabs, C, W), BF16),
            dma((3,)), dma((2, 2)), dma((slabs,)), dma((2, slabs)), dma, dma, dma((3,)), dma((2 * Z,)), dma((2 * Z,)),
            dma((slabs,)), dma((slabs,)), dma((slabs,)), dma((slabs,)),
        ]
        return pl.pallas_call(
            _kernel,
            out_shape=pltpu.VMEM(x.shape, x.dtype),
            in_specs=[hbm] * 7,
            out_specs=pl.BlockSpec(memory_space=pltpu.VMEM),
            scratch_shapes=scratch,
            compiler_params=pltpu.CompilerParams(collective_id=0, has_side_effects=True, vmem_limit_bytes=60 * 2**20),
            name="layer",
        )(x, gain, wq, wk, wv, wo, jnp.asarray(_table(Z * C)))

    tokens, whole = P(("dp", "sp"), None), P(None, None)
    return jax.shard_map(
        step,
        mesh=mesh,
        in_specs=(tokens, P(None), whole, whole, whole, whole),
        out_specs=tokens,
        check_vma=False,
    )
```
